32 devices in a mesh: dp: 16 (over z, x, core), mp: 2 (over y).
Axes of the slice: x: 2, y: 2, z: 4, core: 2. Of those that a mesh axis runs over, the one named last changes fastest.
Arguments:
- tokens: bfloat16 [8192, 8192], P('dp'), may hold values from -6 to 6
- queries: bfloat16 [8192, 64, 128], P('dp', 'mp'), may hold values from -68 to 68
- out_grad: bfloat16 [8192, 64, 128], P('dp', 'mp'), may hold values from -6 to 6
- segment_ids: int32 [16, 512], P('dp'), may hold values from 0 to 3, never falling along the last dimension, each value on 1 to 256 neighbouring positions
- weight_slots: bfloat16 [16384, 8, 2, 128], P('dp', 'mp'), may hold values from -0.0625 to 0.0625
- old_place: int32 [64], replicated, may hold values from 0 to 127, as said below
- new_place: int32 [64], replicated, may hold values from 0 to 127, as said below
Outputs:
- input_grad: bfloat16 [8192, 8192], P('dp', 'mp')
- query_grad: bfloat16 [8192, 64, 128], P('dp', 'mp')
- weight_grad: float32 [16384, 8, 2, 128], P('dp', 'mp')
The draws below stay inside these ranges and needn't reach their ends.
Inputs may be any that keep to these rules, and one draw needn't show every extreme that they name: `old_place`: entries are distinct slot numbers; slot s lies on index s // 8 of dp; some index of dp holds 8 blocks. `new_place`: entries are distinct slot numbers; slot s lies on index s // 8 of dp; some index of dp receives 8 blocks.
All inputs are finite; a program needn't handle non-finite values.
Results may differ from the reference program's by a relative error of at most 0.018.
Values may be sent and summed in bfloat16 or wider, within the bound.
A program may use at most 192 MiB of HBM per device.

```python
import math
import jax
import jax.numpy as jnp
import numpy as np
from jax import lax

D = 8192
QH = 64
KVH = 8
HD = 128
BR = 128
TOK = 512
BLOCKS = 64
SLOTS = 8
TOKENS = 8192
N_DP = 16


def place_blocks(key):
    slot_count = N_DP * SLOTS
    first_key, second_key = jax.random.split(key)
    shuffled = jax.random.permutation(first_key, slot_count).astype(jnp.int32)
    busiest = jax.random.randint(second_key, (), 0, N_DP).astype(jnp.int32)
    owner_dev = jnp.arange(slot_count, dtype=jnp.int32) // SLOTS
    priority = shuffled - (owner_dev == busiest).astype(jnp.int32) * slot_count
    ordered = jnp.argsort(priority, stable=True).astype(jnp.int32)
    return ordered[:BLOCKS]


def draw_old_place(key, part):
    return place_blocks(jax.random.fold_in(key, 11))


def draw_new_place(key, part):
    return place_blocks(jax.random.fold_in(key, 23))


def draw_queries(key, part):
    base_key = jax.random.fold_in(key, 0)
    base = jnp.clip(jax.random.normal(base_key, (TOKENS, QH, HD), jnp.float32), -6.0, 6.0)
    return base.astype(jnp.bfloat16)


def strengthened(drawn, own_key, source, target, blocks, factor):
    owner, partner = [(jnp.arange(drawn.shape[axis_at]) // (drawn.shape[axis_at] // blocks)).reshape([-1 if axis == axis_at else 1 for axis in range(drawn.ndim)]) for axis_at in (source, target)]
    chosen = jax.random.permutation(own_key, blocks)[partner]
    strong = (owner == chosen) | (owner == (partner + blocks // 2) % blocks)
    return jnp.where(strong, factor * drawn, drawn)


def block_scale(own_key, extent, cuts, smallest, top_value):
    level = 1.0
    for dim, parts in cuts:
        heights = jax.random.uniform(jax.random.fold_in(jax.random.fold_in(own_key, 6), dim), (parts,), jnp.float32, smallest / len(cuts), top_value / len(cuts))
        level = level * jnp.repeat(jnp.exp(heights), extent[dim] // parts).reshape((-1,) + (1,) * (len(extent) - 1 - dim))
    return level


def length_profile(number_of, total, reach, skew):
    portions = [(1 << 20) // math.isqrt(standing ** skew) + 1 for standing in range(2, number_of + 1)]
    rest, given = total - reach - (number_of - 1), [1] * (number_of - 1)
    while rest > 0:
        candidates = [i for i in range(number_of - 1) if given[i] < reach]
        whole, budget = sum([portions[i] for i in candidates]), rest
        for i in candidates:
            more = min(reach - given[i], max(1, budget * portions[i] // whole), rest)
            given[i] = given[i] + more
            rest = rest - more
    return np.array([reach] + given)


def uneven_parts(key, count, total, bound, slope):
    if count == 2:
        one = jax.random.randint(key, (), max(1, total - bound), min(bound, total - 1) + 1)
        return jnp.stack([one, total - one])
    sizes = jnp.asarray(length_profile(count, total, bound, slope), jnp.int32)
    pairs = (count - 1) // 2
    source_of, taker = sizes[1:1 + 2 * pairs:2], sizes[2:2 + 2 * pairs:2]
    margin = jnp.minimum(source_of - 1, bound - taker)
    moved = jax.random.randint(jax.random.fold_in(key, 1), (pairs,), 0, 1 << 20) % (margin + 1)
    sizes = sizes.at[1:1 + 2 * pairs:2].set(source_of - moved).at[2:2 + 2 * pairs:2].set(taker + moved)
    return sizes[jax.random.permutation(jax.random.fold_in(key, 2), count)]


def centred(rng, shape, spread, reach, cuts=(), kind=jnp.bfloat16):
    gain = block_scale(rng, shape, cuts, -0.22, 0.18) if cuts else 1.0
    array = jax.random.normal(rng, shape, jnp.float32) * spread * gain
    return jnp.minimum(jnp.maximum(array, -reach), reach).astype(kind)


def heavy_noise(rng, shape, width, reach, cuts, heavy, kind=jnp.bfloat16):
    entries = width * jax.random.normal(rng, shape, jnp.float32)
    if cuts:
        entries = entries * block_scale(rng, shape, cuts, -0.22, 0.18)
    return jnp.clip(strengthened(entries, jax.random.fold_in(rng, 3), *heavy), -reach, reach).astype(kind)


def setup_inputs(seed: int = 0) -> dict:
    streams_of = jax.random.split(jax.random.key(seed), 8)
    tokens = heavy_noise(streams_of[0], (TOKENS, D), 1.0, 6.0, ((0, 16),), (0, 1, 16, 2.0))
    queries = draw_queries(jax.random.fold_in(streams_of[7], 71), 0)
    out_grad = centred(streams_of[2], (TOKENS, QH, HD), 1.0, 6.0, ((0, 16), (1, 2)))
    segment_ids = jax.vmap(lambda own: jnp.searchsorted(jnp.cumsum(uneven_parts(own, 4, TOK, TOK // 2, 0)), jnp.arange(TOK), side="right"))(jax.random.split(streams_of[3], N_DP)).reshape((N_DP, TOK)).astype(jnp.int32)
    weight_slots = centred(streams_of[4], (N_DP * SLOTS * BR, KVH, 2, HD), D ** -0.5, 0.0625, ((0, 16), (1, 2)))
    old_place = draw_old_place(jax.random.fold_in(streams_of[7], 71), 0)
    new_place = draw_new_place(jax.random.fold_in(streams_of[7], 71), 0)
    return dict(tokens=tokens, queries=queries, out_grad=out_grad, segment_ids=segment_ids, weight_slots=weight_slots, old_place=old_place, new_place=new_place)


def attend(tokens, weights, queries, out_grad, seg_row):
    tok_count = tokens.shape[0]
    model_width = weights.shape[0]
    head_count = weights.shape[1]
    head_size = weights.shape[3]
    per_head = queries.shape[1] // head_count
    half_size = head_size // 2
    projected = jnp.dot(tokens, weights.reshape(model_width, head_count * 2 * head_size), preferred_element_type=jnp.float32)
    projected = projected.reshape(tok_count, head_count, 2, head_size)
    frequency = 500000.0 ** (-2.0 * jnp.arange(half_size, dtype=jnp.float32) / head_size)
    angle_tab = jnp.arange(tok_count, dtype=jnp.float32)[:, None] * frequency[None, :]
    cos_tab = jnp.cos(angle_tab)[:, None, :]
    sin_tab = jnp.sin(angle_tab)[:, None, :]
    lower_half = projected[:, :, 0, :half_size]
    upper_half = projected[:, :, 0, half_size:]
    rot_keys = jnp.concatenate([lower_half * cos_tab - upper_half * sin_tab, upper_half * cos_tab + lower_half * sin_tab], axis=-1).astype(jnp.bfloat16)
    values = projected[:, :, 1].astype(jnp.bfloat16)
    inv_root = 1.0 / jnp.sqrt(jnp.float32(head_size))
    query_wide = queries.reshape(tok_count, head_count, per_head, head_size).astype(jnp.float32)
    outgrad_wide = out_grad.reshape(tok_count, head_count, per_head, head_size).astype(jnp.float32)
    key_wide = rot_keys.astype(jnp.float32)
    value_wide = values.astype(jnp.float32)
    scores = jnp.einsum('qhgd,khd->hgqk', query_wide, key_wide) * inv_root
    position = jnp.arange(tok_count)
    allowed = (position[:, None] >= position[None, :]) & (seg_row[:, None] == seg_row[None, :])
    scores = jnp.where(allowed, scores, jnp.float32(-1e+30))
    row_max = lax.optimization_barrier(jnp.max(scores, axis=-1, keepdims=True))
    exp_scores = jnp.exp(scores - row_max)
    attn_prob = exp_scores / lax.optimization_barrier(jnp.sum(exp_scores, axis=-1, keepdims=True))
    prob_half = lax.optimization_barrier(attn_prob.astype(jnp.bfloat16)).astype(jnp.float32)
    attn_out = jnp.einsum('hgqk,khd->qhgd', prob_half, value_wide)
    row_dot = lax.optimization_barrier(jnp.sum(outgrad_wide * attn_out, axis=-1))
    prob_grad = jnp.einsum('qhgd,khd->hgqk', outgrad_wide, value_wide)
    score_grad = attn_prob * (prob_grad - jnp.transpose(row_dot, (1, 2, 0))[..., None])
    score_half = lax.optimization_barrier(score_grad.astype(jnp.bfloat16)).astype(jnp.float32)
    query_grad = (jnp.einsum('hgqk,khd->qhgd', score_half, key_wide) * inv_root).reshape(tok_count, head_count * per_head, head_size).astype(jnp.bfloat16)
    rot_grad = jnp.einsum('hgqk,qhgd->khd', score_half, query_wide) * inv_root
    value_grad = jnp.einsum('hgqk,qhgd->khd', prob_half, outgrad_wide)
    grad_lower = rot_grad[..., :half_size]
    grad_upper = rot_grad[..., half_size:]
    key_grad = jnp.concatenate([grad_lower * cos_tab + grad_upper * sin_tab, grad_upper * cos_tab - grad_lower * sin_tab], axis=-1)
    pair_grad = jnp.stack([key_grad, value_grad], axis=2).astype(jnp.bfloat16)
    return (query_grad, pair_grad)

def reference(tokens, queries, out_grad, segment_ids, weight_slots, old_place, new_place):
    in_block = jnp.arange(BR, dtype=jnp.int32)
    old_index = (old_place.astype(jnp.int32)[:, None] * BR + in_block[None, :]).reshape(-1)
    weights = jnp.take(weight_slots, old_index, axis=0)
    weight_flat = weights.reshape(D, KVH * 2 * HD)

    def per_sequence(grad_acc, inputs):
        seq_tokens, seq_queries, seq_outgrad, seq_ids = inputs
        query_grad, pair_grad = attend(seq_tokens, weights, seq_queries, seq_outgrad, seq_ids)
        pair_flat = pair_grad.reshape(TOK, KVH * 2 * HD)
        seq_part = lax.dot_general(seq_tokens, pair_flat, (((0,), (0,)), ((), ())), preferred_element_type=jnp.float32).astype(jnp.bfloat16)
        grad_acc = grad_acc + lax.optimization_barrier(seq_part).astype(jnp.float32)
        input_grad = lax.dot_general(pair_flat, weight_flat, (((1,), (1,)), ((), ())), preferred_element_type=jnp.float32).astype(jnp.bfloat16)
        return (grad_acc, (input_grad, query_grad))
    stacked = (tokens.reshape(N_DP, TOK, D), queries.reshape(N_DP, TOK, QH, HD), out_grad.reshape(N_DP, TOK, QH, HD), segment_ids)
    grad_sum, (input_grads, query_grads) = lax.scan(per_sequence, jnp.zeros((D, KVH * 2 * HD), jnp.float32), stacked)
    slot_ids = jnp.arange(N_DP * SLOTS, dtype=jnp.int32)
    matched = (new_place.astype(jnp.int32)[None, :] == slot_ids[:, None]).astype(jnp.int32)
    slot_block = lax.optimization_barrier(jnp.sum(matched * jnp.arange(BLOCKS, dtype=jnp.int32)[None, :], axis=1))
    slot_used = lax.optimization_barrier(jnp.sum(matched, axis=1)).astype(jnp.float32)
    row_index = (slot_block[:, None] * BR + in_block[None, :]).reshape(-1)
    row_keep = jnp.repeat(slot_used, BR)
    weight_grad = jnp.take(grad_sum, row_index, axis=0) * row_keep[:, None]
    return (input_grads.reshape(TOKENS, D), query_grads.reshape(TOKENS, QH, HD), weight_grad.reshape(N_DP * SLOTS * BR, KVH, 2, HD))
```

```python
import functools

import jax
import jax.numpy as jnp
from jax import lax
from jax.experimental import pallas as pl
from jax.experimental.pallas import tpu as pltpu
from jax.sharding import PartitionSpec as P

BR = 128
LOG2E = 1.4426950408889634
VMEM_LIMIT = 60 * 1024 * 1024
MESH = pl.DeviceIdType.MESH


def params():
    return pltpu.CompilerParams(
        dimension_semantics=("arbitrary",), vmem_limit_bytes=VMEM_LIMIT
    )


def group_of(count):
    for size in (8, 4, 2):
        if count % size == 0:
            return size
    return 1


def block_specs(group, width):
    return [
        pl.BlockSpec((BR, width), functools.partial(lambda r, i, p: (p[i * group + r], 0), r))
        for r in range(group)
    ]


def project_kernel(group, head_size, place, tok_ref, cos_ref, sin_ref, *refs):
    blocks, out_ref, total = refs[:group], refs[group], refs[group + 1]
    step = pl.program_id(0)

    @pl.when(step == 0)
    def _():
        total[...] = jnp.zeros_like(total)

    w = jnp.concatenate([b[...] for b in blocks], axis=0)
    total[...] += jnp.dot(tok_ref[...], w, preferred_element_type=jnp.float32)

    @pl.when(step == pl.num_programs(0) - 1)
    def _():
        pair = 2 * head_size
        for h in range(total.shape[1] // pair):
            key = total[:, h * pair : h * pair + head_size]
            rot = key * cos_ref[...] + pltpu.roll(key, head_size // 2, 1) * sin_ref[...]
            out_ref[:, h * pair : h * pair + head_size] = rot.astype(jnp.bfloat16)
            value = total[:, h * pair + head_size : (h + 1) * pair]
            out_ref[:, h * pair + head_size : (h + 1) * pair] = value.astype(jnp.bfloat16)


def project(tokens, gathered, place, cos_tab, sin_tab, head_size):
    tok_count = tokens.shape[0]
    width = gathered.shape[1]
    count = place.shape[0]
    group = group_of(count)
    table = pl.BlockSpec((tok_count, head_size), lambda i, p: (0, 0))
    return pl.pallas_call(
        functools.partial(project_kernel, group, head_size),
        out_shape=jax.ShapeDtypeStruct((tok_count, width), jnp.bfloat16),
        grid_spec=pltpu.PrefetchScalarGridSpec(
            num_scalar_prefetch=1,
            grid=(count // group,),
            in_specs=[pl.BlockSpec((tok_count, group * BR), lambda i, p: (0, i)), table, table]
            + block_specs(group, width),
            out_specs=pl.BlockSpec((tok_count, width), lambda i, p: (0, 0)),
            scratch_shapes=[pltpu.VMEM((tok_count, width), jnp.float32)],
        ),
        compiler_params=params(),
        cost_estimate=pl.CostEstimate(
            flops=2 * tok_count * count * BR * width,
            bytes_accessed=2 * (tok_count * count * BR + count * BR * width + tok_count * width),
            transcendentals=0,
        ),
        name="project",
    )(place, tokens, cos_tab, sin_tab, *([gathered] * group))


def attend_kernel(
    per_head, tile, q_ref, og_ref, kv_ref, col_ref, row_ref, cos_ref, sin_ref,
    dq_ref, pair_ref, bias, key_t, rot_acc, val_acc,
):
    tok_count, pair = kv_ref.shape
    hd = pair // 2
    inv_root = 1.0 / (hd ** 0.5)

    @pl.when(pl.program_id(0) == 0)
    def _():
        kpos = lax.broadcasted_iota(jnp.int32, bias.shape, 0)
        qpos = lax.broadcasted_iota(jnp.int32, bias.shape, 1)
        allowed = (kpos <= qpos) & (col_ref[...] == row_ref[...])
        bias[...] = jnp.where(allowed, 0.0, -1e30).astype(jnp.float32)

    key_t[...] = kv_ref[:, :hd].astype(jnp.float32).T.astype(jnp.bfloat16)
    rot_acc[...] = jnp.zeros_like(rot_acc)
    val_acc[...] = jnp.zeros_like(val_acc)

    def head(j, carry):
        lanes = pl.ds(pl.multiple_of(j * hd, hd), hd)
        for t in range(tok_count // tile):
            rows = slice(t * tile, (t + 1) * tile)
            reach = (t + 1) * tile
            q = q_ref[rows, lanes]
            og = og_ref[rows, lanes]
            nt = (((1,), (1,)), ((), ()))
            s = lax.dot_general(kv_ref[:reach, :hd], q, nt, preferred_element_type=jnp.float32)
            s = s * (inv_root * LOG2E) + bias[:reach, rows]
            e = jnp.exp2(s - jnp.max(s, axis=0, keepdims=True))
            p = e * (1.0 / jnp.sum(e, axis=0, keepdims=True))
            pb = p.astype(jnp.bfloat16)
            dp = lax.dot_general(kv_ref[:reach, hd:], og, nt, preferred_element_type=jnp.float32)
            dot = jnp.sum(pb.astype(jnp.float32) * dp, axis=0, keepdims=True)
            ds = (p * (dp - dot)).astype(jnp.bfloat16)
            val_acc[:reach, :] += jnp.dot(pb, og, preferred_element_type=jnp.float32)
            rot_acc[:reach, :] += jnp.dot(ds, q, preferred_element_type=jnp.float32)
            dq = jnp.dot(key_t[:, :reach], ds, preferred_element_type=jnp.float32)
            dq_ref[rows, lanes] = (dq * inv_root).T.astype(jnp.bfloat16)
        return carry

    lax.fori_loop(0, per_head, head, 0, unroll=2)
    g = rot_acc[...] * inv_root
    back = g * cos_ref[...] - pltpu.roll(g, hd // 2, 1) * sin_ref[...]
    pair_ref[:, :hd] = back.astype(jnp.bfloat16)
    pair_ref[:, hd:] = val_acc[...].astype(jnp.bfloat16)


def attend(queries, out_grad, pairs, seg_row, cos_tab, sin_tab, head_count, head_size):
    tok_count, q_width = queries.shape
    per_head = q_width // head_count // head_size
    tile = tok_count // 2 if tok_count % 512 == 0 else tok_count
    slab = pl.BlockSpec((tok_count, per_head * head_size), lambda h: (0, h))
    both = pl.BlockSpec((tok_count, 2 * head_size), lambda h: (0, h))
    table = pl.BlockSpec((tok_count, head_size), lambda h: (0, 0))
    col = pl.BlockSpec((tok_count, 1), lambda h: (0, 0))
    row = pl.BlockSpec((1, tok_count), lambda h: (0, 0))
    return pl.pallas_call(
        functools.partial(attend_kernel, per_head, tile),
        out_shape=(
            jax.ShapeDtypeStruct(queries.shape, jnp.bfloat16),
            jax.ShapeDtypeStruct(pairs.shape, jnp.bfloat16),
        ),
        grid=(head_count,),
        in_specs=[slab, slab, both, col, row, table, table],
        out_specs=(slab, both),
        scratch_shapes=[
            pltpu.VMEM((tok_count, tok_count), jnp.float32),
            pltpu.VMEM((head_size, tok_count), jnp.bfloat16),
            pltpu.VMEM((tok_count, head_size), jnp.float32),
            pltpu.VMEM((tok_count, head_size), jnp.float32),
        ],
        compiler_params=params(),
        cost_estimate=pl.CostEstimate(
            flops=10 * tok_count * tok_count * q_width,
            bytes_accessed=6 * tok_count * q_width + 4 * tok_count * pairs.shape[1],
            transcendentals=tok_count * tok_count * q_width // head_size,
        ),
        name="attend",
    )(queries, out_grad, pairs, seg_row.reshape(-1, 1), seg_row, cos_tab, sin_tab)


def chip_at(chips, position):
    return jnp.where(position < chips // 2, 2 * position, 2 * (chips - 1 - position) + 1)


def scatter_kernel(
    chips, subs, block_of, used, tok_ref, pair_ref, out_ref,
    part_out, part_in, ring_out, ring_in, final, swap_out, swap_in,
    part_sent, part_got, ring_sent, ring_got, swap_sent, swap_got,
):
    dp_count = 2 * chips
    me = lax.axis_index("dp")
    chip, core = me // 2, lax.rem(me, 2)
    half = chip // 2
    place = jnp.where(lax.rem(chip, 2) == 0, half, chips - 1 - half)
    ahead = 2 * chip_at(chips, lax.rem(place + 1, chips)) + core
    behind = 2 * chip_at(chips, lax.rem(place + chips - 1, chips)) + core
    partner = 2 * chip + 1 - core
    piece_rows, tok_count = tok_ref.shape[1:]
    cols = pair_ref.shape[1] // 2
    sub = piece_rows // subs
    slots, short = swap_out.shape[1:3]

    barrier = pltpu.get_barrier_semaphore()

    @pl.loop(1, dp_count)
    def _(k):
        pl.semaphore_signal(
            barrier, inc=1, device_id={"dp": lax.rem(me + k, dp_count)}, device_id_type=MESH
        )

    pl.semaphore_wait(barrier, dp_count - 1)

    def goal(way, step):
        offset = chips - 1 - step if way == 0 else 1 + step
        return chip_at(chips, lax.rem(place + offset, chips))

    def product(piece, rows, way):
        return jnp.dot(
            tok_ref[piece, rows, :], pair_ref[:, way * cols : (way + 1) * cols],
            preferred_element_type=jnp.float32,
        )

    def part_copy(way, step):
        return pltpu.make_async_remote_copy(
            src_ref=part_out.at[way, step], dst_ref=part_in.at[way, step],
            send_sem=part_sent.at[way, step], recv_sem=part_got.at[way, step],
            device_id={"dp": partner}, device_id_type=MESH,
        )

    def ring_copy(way, step, u):
        rows = pl.ds(u * sub, sub)
        return pltpu.make_async_remote_copy(
            src_ref=ring_out.at[way, step, rows], dst_ref=ring_in.at[way, step, rows],
            send_sem=ring_sent.at[way, step, u], recv_sem=ring_got.at[way, step, u],
            device_id={"dp": ahead if way == 0 else behind}, device_id_type=MESH,
        )

    def send_part(step):
        for way in range(2):
            piece = 2 * goal(way, step) + 1 - core
            for u in range(subs):
                rows = slice(u * sub, (u + 1) * sub)
                part_out[way, step, rows, :] = product(piece, rows, way).astype(jnp.bfloat16)
            part_copy(way, step).start()

    def ring_step(step, first, last):
        for way in range(2):
            part_copy(way, step).wait_recv()
        for u in range(subs):
            rows = slice(u * sub, (u + 1) * sub)
            for way in range(2):
                piece = 2 * goal(way, step) + core
                total = product(piece, rows, way) + part_in[way, step, rows, :].astype(jnp.float32)
                if not first:
                    ring_copy(way, step - 1, u).wait_recv()
                    total = total + ring_in[way, step - 1, rows, :].astype(jnp.float32)
                if last:
                    blocks = pl.ds(u * (sub // short), sub // short)
                    final[blocks, :, way * cols : (way + 1) * cols] = total.reshape(
                        sub // short, short, cols
                    ).astype(jnp.bfloat16)
                else:
                    ring_out[way, step, rows, :] = total.astype(jnp.bfloat16)
                    ring_copy(way, step, u).start()

    send_part(0)
    send_part(1)
    ring_step(0, True, False)

    @pl.loop(1, chips - 1)
    def _(step):
        send_part(step + 1)
        ring_step(step, False, False)

    ring_step(chips - 1, False, True)

    def swap_copy(k):
        peer = lax.rem(me + k, dp_count)
        return pltpu.make_async_remote_copy(
            src_ref=swap_out.at[peer], dst_ref=swap_in.at[me],
            send_sem=swap_sent.at[k], recv_sem=swap_got.at[k],
            device_id={"dp": peer}, device_id_type=MESH,
        )

    def fill(peer):
        for i in range(slots):
            slot = peer * slots + i
            rows = final[block_of[slot]]
            swap_out[peer, i] = jnp.where(used[slot] != 0, rows, jnp.zeros_like(rows))

    @pl.loop(1, dp_count)
    def _(k):
        fill(lax.rem(me + k, dp_count))
        swap_copy(k).start()

    fill(me)
    out_ref[:, pl.ds(me, 1)] = swap_out[me].astype(jnp.float32)[:, None]

    @pl.loop(1, dp_count)
    def _(k):
        swap_copy(k).wait_recv()
        origin = lax.rem(me + dp_count - k, dp_count)
        out_ref[:, pl.ds(origin, 1)] = swap_in[origin].astype(jnp.float32)[:, None]

    @pl.loop(1, dp_count)
    def _(k):
        swap_copy(k).wait_send()

    @pl.loop(0, chips)
    def _(step):
        for way in range(2):
            part_copy(way, step).wait_send()

    @pl.loop(0, chips - 1)
    def _(step):
        for way in range(2):
            for u in range(subs):
                ring_copy(way, step, u).wait_send()


def scatter_sum(tok_pieces, pairs, block_of, used, dp_count):
    chips = dp_count // 2
    width = pairs.shape[1]
    piece_rows = tok_pieces.shape[1]
    slots = block_of.shape[0] // dp_count
    short = BR // dp_count
    subs = 4
    whole = pl.BlockSpec(memory_space=pltpu.VMEM)
    scalars = pl.BlockSpec(memory_space=pltpu.SMEM)
    cols = width // 2
    bf = jnp.bfloat16
    sent = 2 * 2 * (chips - 1) * piece_rows * cols * 2
    return pl.pallas_call(
        functools.partial(scatter_kernel, chips, subs),
        out_shape=jax.ShapeDtypeStruct((slots, dp_count, short, width), jnp.float32),
        in_specs=[scalars, scalars, whole, whole],
        out_specs=whole,
        scratch_shapes=[
            pltpu.VMEM((2, chips, piece_rows, cols), bf),
            pltpu.VMEM((2, chips, piece_rows, cols), bf),
            pltpu.VMEM((2, chips - 1, piece_rows, cols), bf),
            pltpu.VMEM((2, chips - 1, piece_rows, cols), bf),
            pltpu.VMEM((piece_rows // short, short, width), bf),
            pltpu.VMEM((dp_count, slots, short, width), bf),
            pltpu.VMEM((dp_count, slots, short, width), bf),
            pltpu.SemaphoreType.DMA((2, chips)),
            pltpu.SemaphoreType.DMA((2, chips)),
            pltpu.SemaphoreType.DMA((2, chips - 1, subs)),
            pltpu.SemaphoreType.DMA((2, chips - 1, subs)),
            pltpu.SemaphoreType.DMA((dp_count,)),
            pltpu.SemaphoreType.DMA((dp_count,)),
        ],
        compiler_params=pltpu.CompilerParams(
            collective_id=0, has_side_effects=True, vmem_limit_bytes=VMEM_LIMIT
        ),
        cost_estimate=pl.CostEstimate(
            flops=2 * tok_pieces.size * width * 8, bytes_accessed=sent, transcendentals=0
        ),
        name="scatter_sum",
    )(block_of, used, tok_pieces, pairs)


def input_kernel(group, add, place, pair_ref, *refs):
    blocks, out_ref = refs[:group], refs[-1]
    w = jnp.concatenate([b[...] for b in blocks], axis=0)
    total = lax.dot_general(
        pair_ref[...], w, (((1,), (1,)), ((), ())), preferred_element_type=jnp.float32
    )
    if add:
        total = total + refs[group][...].astype(jnp.float32)
    out_ref[...] = total.astype(jnp.bfloat16)


def input_part(pairs, gathered, place, other=None):
    tok_count, width = pairs.shape
    count = place.shape[0]
    group = group_of(count)
    wide = pl.BlockSpec((tok_count, group * BR), lambda i, p: (0, i))
    add = other is not None
    return pl.pallas_call(
        functools.partial(input_kernel, group, add),
        out_shape=jax.ShapeDtypeStruct((tok_count, count * BR), jnp.bfloat16),
        grid_spec=pltpu.PrefetchScalarGridSpec(
            num_scalar_prefetch=1,
            grid=(count // group,),
            in_specs=[pl.BlockSpec(pairs.shape, lambda i, p: (0, 0))]
            + block_specs(group, width)
            + ([wide] if add else []),
            out_specs=wide,
        ),
        compiler_params=params(),
        cost_estimate=pl.CostEstimate(
            flops=2 * tok_count * width * count * BR,
            bytes_accessed=2 * (count * BR * width + 2 * tok_count * count * BR),
            transcendentals=0,
        ),
        name="input_own" if add else "input_other",
    )(place, pairs, *([gathered] * group), *((other,) if add else ()))


def local(tokens, queries, out_grad, segment_ids, weight_slots, old_place, new_place):
    tok_count = tokens.shape[0]
    slot_rows, head_count, _, head_size = weight_slots.shape
    width = head_count * 2 * head_size
    dp_count = lax.axis_size("dp")
    mp_count = lax.axis_size("mp")
    slot_total = dp_count * (slot_rows // BR)
    block_count = old_place.shape[0]

    gathered = lax.all_gather(weight_slots.reshape(slot_rows, width), "dp", axis=0, tiled=True)

    half = head_size // 2
    frequency = 500000.0 ** (-2.0 * jnp.arange(half, dtype=jnp.float32) / head_size)
    angle = jnp.arange(tok_count, dtype=jnp.float32)[:, None] * frequency[None, :]
    cos_half, sin_half = jnp.cos(angle), jnp.sin(angle)
    cos_tab = jnp.concatenate([cos_half, cos_half], axis=1)
    sin_tab = jnp.concatenate([-sin_half, sin_half], axis=1)

    pairs = project(tokens, gathered, old_place, cos_tab, sin_tab, head_size)
    query_grad, pair_grad = attend(
        queries.reshape(tok_count, -1), out_grad.reshape(tok_count, -1), pairs, segment_ids,
        cos_tab, sin_tab, head_count, head_size,
    )

    slot_ids = jnp.arange(slot_total, dtype=jnp.int32)
    matched = (new_place[None, :] == slot_ids[:, None]).astype(jnp.int32)
    block_of = jnp.sum(matched * jnp.arange(block_count, dtype=jnp.int32)[None, :], axis=1)
    used = jnp.sum(matched, axis=1)
    short = BR // dp_count
    tok_pieces = tokens.reshape(tok_count, block_count, dp_count, short).transpose(2, 1, 3, 0)
    tok_pieces = tok_pieces.reshape(dp_count, block_count * short, tok_count)

    me = lax.axis_index("mp")
    share = old_place.reshape(mp_count, block_count // mp_count)
    total = None
    for gap in range(1, mp_count):
        target = lax.rem(me + gap, mp_count)
        places = lax.dynamic_index_in_dim(share, target, 0, keepdims=False)
        piece = input_part(pair_grad, gathered, places)
        ring = [(i, (i + gap) % mp_count) for i in range(mp_count)]
        arrived = lax.ppermute(piece, "mp", ring)
        total = arrived if total is None else total + arrived
    weight_grad = scatter_sum(tok_pieces, pair_grad, block_of, used, dp_count)
    mine = lax.dynamic_index_in_dim(share, me, 0, keepdims=False)
    input_grad = input_part(pair_grad, gathered, mine, total)
    return (
        input_grad,
        query_grad.reshape(queries.shape),
        weight_grad.reshape(slot_rows, head_count, 2, head_size),
    )


def solution(mesh):
    return jax.shard_map(
        local,
        mesh=mesh,
        in_specs=(
            P("dp", None),
            P("dp", "mp", None),
            P("dp", "mp", None),
            P("dp", None),
            P("dp", "mp", None, None),
            P(),
            P(),
        ),
        out_specs=(P("dp", "mp"), P("dp", "mp", None), P("dp", "mp", None, None)),
        check_vma=False,
    )
```

```python
import functools

import jax
import jax.numpy as jnp
from jax import lax
from jax.experimental import pallas as pl
from jax.experimental.pallas import tpu as pltpu
from jax.sharding import PartitionSpec as P

BR = 128
LOG2E = 1.4426950408889634
VMEM_LIMIT = 60 * 1024 * 1024
MESH = pl.DeviceIdType.MESH


def params():
    return pltpu.CompilerParams(
        dimension_semantics=("arbitrary",), vmem_limit_bytes=VMEM_LIMIT
    )


def group_of(count):
    for size in (8, 4, 2):
        if count % size == 0:
            return size
    return 1


def chip_at(chips, position):
    return jnp.where(position < chips // 2, 2 * position, 2 * (chips - 1 - position) + 1)


def position_of(chips, chip):
    return jnp.where(lax.rem(chip, 2) == 0, chip // 2, chips - 1 - chip // 2)


def meet(dp_count, me):
    barrier = pltpu.get_barrier_semaphore()

    @pl.loop(1, dp_count)
    def _(k):
        pl.semaphore_signal(
            barrier, inc=1, device_id={"dp": lax.rem(me + k, dp_count)}, device_id_type=MESH
        )

    pl.semaphore_wait(barrier, dp_count - 1)


def remote(src, dst, sent, got, peer):
    return pltpu.make_async_remote_copy(
        src_ref=src, dst_ref=dst, send_sem=sent, recv_sem=got,
        device_id={"dp": peer}, device_id_type=MESH,
    )


def gather_kernel(
    chips, heads, subs, tile, place, slots_ref, tok_hbm, q_hbm, og_hbm, col_ref, row_ref,
    cos_ref, sin_ref, dq_ref, pair_ref, w_hbm, tokt_hbm,
    tok, q_ref, og_ref, tokt, w, got, total, kv, bias, key_t, rot_acc, val_acc,
    load_sem, save_sem, swap_sent, swap_got, ring_sent, ring_got, pass_sent, pass_got,
):
    dp_count = 2 * chips
    hops = chips // 2
    me = lax.axis_index("dp")
    core = lax.rem(me, 2)
    spot = position_of(chips, me // 2)
    partner = me + 1 - 2 * core
    groups, blocks, splits, rows, lane = w.shape
    per = chips // groups
    slots = slots_ref.shape[0]
    tok_count, hd = tok.shape[0], lane
    per_head = q_ref.shape[1] // heads // hd
    near = (
        2 * chip_at(chips, lax.rem(spot + 1, chips)) + core,
        2 * chip_at(chips, lax.rem(spot + chips - 1, chips)) + core,
    )
    size = blocks // subs
    inv_root = 1.0 / (hd ** 0.5)

    loads = [
        pltpu.make_async_copy(src, dst, load_sem.at[i])
        for i, (src, dst) in enumerate(((tok_hbm, tok), (q_hbm, q_ref), (og_hbm, og_ref)))
    ]
    for load in loads:
        load.start()

    def part(position, owner):
        return position // per, lax.rem(position, per) * 2 + owner

    meet(dp_count, me)

    def swap_copy(k):
        peer = lax.rem(me + k, dp_count)
        group, split = part(position_of(chips, peer // 2), lax.rem(peer, 2))
        src = slots_ref.at[
            :, pl.ds(pl.multiple_of(split * rows, rows), rows),
            pl.ds(pl.multiple_of(group * lane, lane), lane),
        ]
        return remote(src, got.at[me], swap_sent.at[k], swap_got.at[k], peer)

    @pl.loop(1, dp_count)
    def _(k):
        swap_copy(k).start()

    my_group, my_split = part(spot, core)
    own_rows = pl.ds(pl.multiple_of(my_split * rows, rows), rows)
    own_lanes = pl.ds(pl.multiple_of(my_group * lane, lane), lane)
    got[me] = slots_ref[:, own_rows, own_lanes]

    kpos = lax.broadcasted_iota(jnp.int32, bias.shape, 0)
    qpos = lax.broadcasted_iota(jnp.int32, bias.shape, 1)
    allowed = (kpos <= qpos) & (col_ref[...] == row_ref[...])
    bias[...] = jnp.where(allowed, 0.0, -1e30).astype(jnp.float32)

    for load in loads:
        load.wait()

    @pl.loop(0, blocks)
    def _(b):
        cols = tok[:, pl.ds(pl.multiple_of(b * BR, BR), BR)]
        flipped = cols.astype(jnp.float32).T
        tokt[b] = flipped.reshape(splits, rows, tok_count).astype(jnp.bfloat16)

    save_tok = pltpu.make_async_copy(tokt, tokt_hbm, save_sem.at[groups])
    save_tok.start()

    @pl.loop(1, dp_count)
    def _(k):
        swap_copy(k).wait_recv()

    def piece(origin, owner, u):
        group, split = part(origin, owner)
        return w.at[group, pl.ds(u * size, size), split]

    def ring_copy(way, hop, u):
        origin = lax.rem(spot + hop if way else spot - hop + chips, chips)
        ref = piece(origin, core, u)
        peer = near[1] if way else near[0]
        return remote(ref, ref, ring_sent.at[way, hop - 1, u], ring_got.at[way, hop - 1, u], peer)

    def forward(way, hop, u):
        origin = lax.rem(spot + hop - 1 if way else spot - hop + 1 + chips, chips)
        ref = piece(origin, core, u)
        peer = near[1] if way else near[0]
        return remote(ref, ref, ring_sent.at[way, hop - 1, u], ring_got.at[way, hop - 1, u], peer)

    def pass_copy(origin, owner, u):
        ref = piece(origin, owner, u)
        return remote(ref, ref, pass_sent.at[origin, u], pass_got.at[origin, u], partner)

    def carried(way, hop, u):
        mine = (u < subs // 2) if way == 0 else (u >= subs // 2)
        return (hop < hops) | ((hop == hops) & mine)

    @pl.loop(0, subs)
    def _(u):
        for i in range(size):
            b = u * size + i
            slot = place[b]
            w[my_group, b, my_split] = got[slot // slots, lax.rem(slot, slots)]
        for way in range(2):
            @pl.when(carried(way, 1, u))
            def _():
                forward(way, 1, u).start()
        pass_copy(spot, core, u).start()

    def receive(hop, u):
        for way in range(2):
            @pl.when(carried(way, hop, u))
            def _():
                ring_copy(way, hop, u).wait_recv()
                origin = lax.rem(spot + hop if way else spot - hop + chips, chips)
                pass_copy(origin, core, u).start()

                @pl.when((hop < hops) & carried(way, hop + 1, u))
                def _():
                    forward(way, hop + 1, u).start()

    def shared(origin):
        @pl.loop(0, subs)
        def _(u):
            pass_copy(origin, 1 - core, u).wait_recv()

    def save_copy(group):
        return pltpu.make_async_copy(w.at[group], w_hbm.at[group], save_sem.at[group])

    def begin(head):
        for g in range(2):
            save_copy(2 * head + g).start()
        total[...] = jnp.zeros_like(total)
        step = group_of(blocks)

        @pl.loop(0, blocks // step)
        def _(i):
            ws = [
                w[2 * head + g, pl.ds(i * step, step)].reshape(step * splits * rows, lane)
                for g in range(2)
            ]
            cols = pl.ds(pl.multiple_of(i * step * BR, step * BR), step * BR)
            total[...] += jnp.dot(
                tok[:, cols], jnp.concatenate(ws, axis=1), preferred_element_type=jnp.float32
            )

        key = total[:, :hd]
        rot = key * cos_ref[...] + pltpu.roll(key, hd // 2, 1) * sin_ref[...]
        rot = rot.astype(jnp.bfloat16)
        kv[:, :hd] = rot
        kv[:, hd:] = total[:, hd:].astype(jnp.bfloat16)
        key_t[...] = rot.astype(jnp.float32).T.astype(jnp.bfloat16)
        rot_acc[...] = jnp.zeros_like(rot_acc)
        val_acc[...] = jnp.zeros_like(val_acc)

    def unit(head, j):
        lanes = pl.ds(pl.multiple_of((head * per_head + j) * hd, hd), hd)
        for t in range(tok_count // tile):
            span = slice(t * tile, (t + 1) * tile)
            reach = (t + 1) * tile
            q = q_ref[span, lanes]
            og = og_ref[span, lanes]
            nt = (((1,), (1,)), ((), ()))
            s = lax.dot_general(kv[:reach, :hd], q, nt, preferred_element_type=jnp.float32)
            s = s * (inv_root * LOG2E) + bias[:reach, span]
            e = jnp.exp2(s - jnp.max(s, axis=0, keepdims=True))
            p = e * (1.0 / jnp.sum(e, axis=0, keepdims=True))
            pb = p.astype(jnp.bfloat16)
            dp = lax.dot_general(kv[:reach, hd:], og, nt, preferred_element_type=jnp.float32)
            dot = jnp.sum(pb.astype(jnp.float32) * dp, axis=0, keepdims=True)
            ds = (p * (dp - dot)).astype(jnp.bfloat16)
            val_acc[:reach, :] += jnp.dot(pb, og, preferred_element_type=jnp.float32)
            rot_acc[:reach, :] += jnp.dot(ds, q, preferred_element_type=jnp.float32)
            dq = jnp.dot(key_t[:, :reach], ds, preferred_element_type=jnp.float32)
            dq_ref[span, lanes] = (dq * inv_root).T.astype(jnp.bfloat16)

    def finish(head):
        g = rot_acc[...] * inv_root
        back = g * cos_ref[...] - pltpu.roll(g, hd // 2, 1) * sin_ref[...]
        at = pl.multiple_of(head * 2 * hd, 2 * hd)
        pair_ref[:, pl.ds(at, hd)] = back.astype(jnp.bfloat16)
        pair_ref[:, pl.ds(at + hd, hd)] = val_acc[...].astype(jnp.bfloat16)

    if groups == chips and heads == hops and per_head % subs == 0:
        def head_at(k):
            side = jnp.where(lax.rem(k + spot, 2) == 0, 1, -1)
            return lax.rem(spot // 2 + side * ((k + 1) // 2) + 2 * heads, heads)

        @pl.loop(0, hops + 1)
        def _(t):
            head = head_at(jnp.maximum(t - 1, 0))

            @pl.when(t >= 1)
            def _():
                shared(2 * head)
                shared(2 * head + 1)
                begin(head)

            @pl.loop(0, subs)
            def _(u):
                @pl.when(t < hops)
                def _():
                    receive(t + 1, u)

                @pl.when(t >= 1)
                def _():
                    for i in range(per_head // subs):
                        unit(head, u * (per_head // subs) + i)

            @pl.when(t >= 1)
            def _():
                finish(head)
    else:
        @pl.loop(0, hops)
        def _(t):
            @pl.loop(0, subs)
            def _(u):
                receive(t + 1, u)

        @pl.loop(0, chips)
        def _(origin):
            shared(origin)

        @pl.loop(0, heads)
        def _(head):
            begin(head)

            @pl.loop(0, per_head)
            def _(j):
                unit(head, j)

            finish(head)

    @pl.loop(1, dp_count)
    def _(k):
        swap_copy(k).wait_send()

    @pl.loop(0, subs)
    def _(u):
        @pl.loop(0, chips)
        def _(origin):
            pass_copy(origin, core, u).wait_send()

        @pl.loop(1, hops + 1)
        def _(hop):
            for way in range(2):
                @pl.when(carried(way, hop, u))
                def _():
                    forward(way, hop, u).wait_send()

    @pl.loop(0, groups)
    def _(group):
        save_copy(group).wait()

    save_tok.wait()


def gather_attend(place, slots, tokens, queries, out_grad, seg_row, cos_tab, sin_tab, head_count, dp_count):
    slot_count, _, width = slots.shape
    tok_count, q_width = queries.shape
    chips = dp_count // 2
    lane = width // head_count // 2
    groups = 2 * head_count
    blocks = place.shape[0]
    splits = dp_count // groups
    rows = BR // splits
    subs = 8
    hops = chips // 2
    tile = tok_count // 2 if tok_count % 512 == 0 else tok_count
    bf = jnp.bfloat16
    f32 = jnp.float32
    whole = pl.BlockSpec(memory_space=pltpu.VMEM)
    far = pl.BlockSpec(memory_space=pl.ANY)
    dma = pltpu.SemaphoreType.DMA
    return pl.pallas_call(
        functools.partial(gather_kernel, chips, head_count, subs, tile),
        out_shape=(
            jax.ShapeDtypeStruct((tok_count, q_width), bf),
            jax.ShapeDtypeStruct((tok_count, width), bf),
            jax.ShapeDtypeStruct((groups, blocks, splits, rows, lane), bf),
            jax.ShapeDtypeStruct((blocks, splits, rows, tok_count), bf),
        ),
        in_specs=[pl.BlockSpec(memory_space=pltpu.SMEM), whole, far, far, far] + [whole] * 4,
        out_specs=(whole, whole, far, far),
        scratch_shapes=[
            pltpu.VMEM(tokens.shape, bf),
            pltpu.VMEM(queries.shape, bf),
            pltpu.VMEM(queries.shape, bf),
            pltpu.VMEM((blocks, splits, rows, tok_count), bf),
            pltpu.VMEM((groups, blocks, splits, rows, lane), bf),
            pltpu.VMEM((dp_count, slot_count, rows, lane), bf),
            pltpu.VMEM((tok_count, 2 * lane), f32),
            pltpu.VMEM((tok_count, 2 * lane), bf),
            pltpu.VMEM((tok_count, tok_count), f32),
            pltpu.VMEM((lane, tok_count), bf),
            pltpu.VMEM((tok_count, lane), f32),
            pltpu.VMEM((tok_count, lane), f32),
            dma((3,)),
            dma((groups + 1,)),
            dma((dp_count,)),
            dma((dp_count,)),
            dma((2, hops, subs)),
            dma((2, hops, subs)),
            dma((chips, subs)),
            dma((chips, subs)),
        ],
        compiler_params=pltpu.CompilerParams(
            collective_id=1, has_side_effects=True, vmem_limit_bytes=VMEM_LIMIT
        ),
        cost_estimate=pl.CostEstimate(
            flops=10 * tok_count * tok_count * q_width, bytes_accessed=10**8,
            transcendentals=tok_count * tok_count * q_width // lane,
        ),
        name="gather_attend",
    )(place, slots, tokens, queries, out_grad, seg_row.reshape(-1, 1), seg_row, cos_tab, sin_tab)


def scatter_kernel(
    chips, subs, block_of, used, tok_ref, pair_ref, out_ref,
    part_out, part_in, ring_out, ring_in, final, swap_out, swap_in,
    part_sent, part_got, ring_sent, ring_got, swap_sent, swap_got,
):
    dp_count = 2 * chips
    me = lax.axis_index("dp")
    core = lax.rem(me, 2)
    spot = position_of(chips, me // 2)
    ahead = 2 * chip_at(chips, lax.rem(spot + 1, chips)) + core
    behind = 2 * chip_at(chips, lax.rem(spot + chips - 1, chips)) + core
    partner = me + 1 - 2 * core
    blocks, splits, rows, tok_count = tok_ref.shape
    lane = final.shape[2]
    groups = pair_ref.shape[1] // lane
    per = chips // groups
    half = blocks // 2
    size = half // subs
    slots = swap_out.shape[1]

    meet(dp_count, me)

    def goal(way, step):
        return lax.rem(spot + (chips - 1 - step if way == 0 else 1 + step), chips)

    def product(way, step, owner, u):
        position = goal(way, step)
        split = lax.rem(position, per) * 2 + owner
        left = tok_ref[way * half + u * size : way * half + (u + 1) * size, split]
        lanes = pl.ds(pl.multiple_of((position // per) * lane, lane), lane)
        return jnp.dot(
            left.reshape(size * rows, tok_count), pair_ref[:, lanes],
            preferred_element_type=jnp.float32,
        ).reshape(size, rows, lane)

    def part_copy(way, step):
        return remote(
            part_out.at[way, step], part_in.at[way, step],
            part_sent.at[way, step], part_got.at[way, step], partner,
        )

    def ring_copy(way, step, u):
        at = pl.ds(u * size, size)
        return remote(
            ring_out.at[way, step, at], ring_in.at[way, step, at],
            ring_sent.at[way, step, u], ring_got.at[way, step, u],
            ahead if way == 0 else behind,
        )

    def send_part(step):
        for way in range(2):
            for u in range(subs):
                at = slice(u * size, (u + 1) * size)
                part_out[way, step, at] = product(way, step, 1 - core, u).astype(jnp.bfloat16)
            part_copy(way, step).start()

    def ring_step(step, first, last):
        for way in range(2):
            part_copy(way, step).wait_recv()
        for u in range(subs):
            at = slice(u * size, (u + 1) * size)
            for way in range(2):
                total = product(way, step, core, u) + part_in[way, step, at].astype(jnp.float32)
                if not first:
                    ring_copy(way, step - 1, u).wait_recv()
                    total = total + ring_in[way, step - 1, at].astype(jnp.float32)
                if last:
                    final[way * half + u * size : way * half + (u + 1) * size] = total.astype(
                        jnp.bfloat16
                    )
                else:
                    ring_out[way, step, at] = total.astype(jnp.bfloat16)
                    ring_copy(way, step, u).start()

    send_part(0)
    send_part(1)
    ring_step(0, True, False)

    @pl.loop(1, chips - 1)
    def _(step):
        send_part(step + 1)
        ring_step(step, False, False)

    ring_step(chips - 1, False, True)

    def swap_copy(k):
        peer = lax.rem(me + k, dp_count)
        return remote(swap_out.at[peer], swap_in.at[me], swap_sent.at[k], swap_got.at[k], peer)

    def fill(peer):
        for i in range(slots):
            slot = peer * slots + i
            taken = final[block_of[slot]]
            swap_out[peer, i] = jnp.where(used[slot] != 0, taken, jnp.zeros_like(taken))

    def place_in(origin, value):
        position = position_of(chips, origin // 2)
        split = lax.rem(position, per) * 2 + lax.rem(origin, 2)
        at = pl.ds(pl.multiple_of(split * rows, rows), rows)
        lanes = pl.ds(pl.multiple_of((position // per) * lane, lane), lane)
        out_ref[:, at, lanes] = value.astype(jnp.float32)

    @pl.loop(1, dp_count)
    def _(k):
        fill(lax.rem(me + k, dp_count))
        swap_copy(k).start()

    fill(me)
    place_in(me, swap_out[me])

    @pl.loop(1, dp_count)
    def _(k):
        swap_copy(k).wait_recv()
        origin = lax.rem(me + dp_count - k, dp_count)
        place_in(origin, swap_in[origin])

    @pl.loop(1, dp_count)
    def _(k):
        swap_copy(k).wait_send()

    @pl.loop(0, chips)
    def _(step):
        for way in range(2):
            part_copy(way, step).wait_send()

    @pl.loop(0, chips - 1)
    def _(step):
        for way in range(2):
            for u in range(subs):
                ring_copy(way, step, u).wait_send()


def scatter_sum(tok_pieces, pairs, block_of, used, dp_count):
    chips = dp_count // 2
    width = pairs.shape[1]
    blocks, splits, rows, tok_count = tok_pieces.shape
    lane = width * splits // dp_count
    slots = block_of.shape[0] // dp_count
    subs = 4
    whole = pl.BlockSpec(memory_space=pltpu.VMEM)
    scalars = pl.BlockSpec(memory_space=pltpu.SMEM)
    half = blocks // 2
    bf = jnp.bfloat16
    dma = pltpu.SemaphoreType.DMA
    return pl.pallas_call(
        functools.partial(scatter_kernel, chips, subs),
        out_shape=jax.ShapeDtypeStruct((slots, BR, width), jnp.float32),
        in_specs=[scalars, scalars, whole, whole],
        out_specs=whole,
        scratch_shapes=[
            pltpu.VMEM((2, chips, half, rows, lane), bf),
            pltpu.VMEM((2, chips, half, rows, lane), bf),
            pltpu.VMEM((2, chips - 1, half, rows, lane), bf),
            pltpu.VMEM((2, chips - 1, half, rows, lane), bf),
            pltpu.VMEM((blocks, rows, lane), bf),
            pltpu.VMEM((dp_count, slots, rows, lane), bf),
            pltpu.VMEM((dp_count, slots, rows, lane), bf),
            dma((2, chips)),
            dma((2, chips)),
            dma((2, chips - 1, subs)),
            dma((2, chips - 1, subs)),
            dma((dp_count,)),
            dma((dp_count,)),
        ],
        compiler_params=pltpu.CompilerParams(
            collective_id=0, has_side_effects=True, vmem_limit_bytes=VMEM_LIMIT
        ),
        cost_estimate=pl.CostEstimate(
            flops=16 * tok_pieces.size * width, bytes_accessed=10**8, transcendentals=0
        ),
        name="scatter_sum",
    )(block_of, used, tok_pieces, pairs)


def input_kernel(add, owner, pair_ref, w_ref, *refs):
    out_ref = refs[-1]
    w = jnp.concatenate([w_ref[g] for g in range(w_ref.shape[0])], axis=1)
    total = lax.dot_general(
        pair_ref[...], w, (((1,), (1,)), ((), ())), preferred_element_type=jnp.float32
    )
    if add:
        total = total + refs[0][...].astype(jnp.float32)
    out_ref[...] = total.astype(jnp.bfloat16)


def input_part(pairs, gathered, owner, count, other=None):
    tok_count, width = pairs.shape
    groups, _, lane = gathered.shape
    deep = group_of(count) * BR
    steps = count * BR // deep
    wide = pl.BlockSpec((tok_count, deep), lambda i, p: (0, i))
    add = other is not None
    return pl.pallas_call(
        functools.partial(input_kernel, add),
        out_shape=jax.ShapeDtypeStruct((tok_count, count * BR), jnp.bfloat16),
        grid_spec=pltpu.PrefetchScalarGridSpec(
            num_scalar_prefetch=1,
            grid=(steps,),
            in_specs=[
                pl.BlockSpec(pairs.shape, lambda i, p: (0, 0)),
                pl.BlockSpec((groups, deep, lane), lambda i, p: (0, p[0] * steps + i, 0)),
            ]
            + ([wide] if add else []),
            out_specs=wide,
        ),
        compiler_params=params(),
        cost_estimate=pl.CostEstimate(
            flops=2 * tok_count * width * count * BR,
            bytes_accessed=2 * (count * BR * width + 2 * tok_count * count * BR),
            transcendentals=0,
        ),
        name="input_own" if add else "input_other",
    )(owner.reshape(1), pairs, gathered, *((other,) if add else ()))


def local(tokens, queries, out_grad, segment_ids, weight_slots, old_place, new_place):
    tok_count = tokens.shape[0]
    slot_rows, head_count, _, head_size = weight_slots.shape
    width = head_count * 2 * head_size
    dp_count = lax.axis_size("dp")
    mp_count = lax.axis_size("mp")
    slot_total = dp_count * (slot_rows // BR)
    block_count = old_place.shape[0]

    half = head_size // 2
    frequency = 500000.0 ** (-2.0 * jnp.arange(half, dtype=jnp.float32) / head_size)
    angle = jnp.arange(tok_count, dtype=jnp.float32)[:, None] * frequency[None, :]
    cos_half, sin_half = jnp.cos(angle), jnp.sin(angle)
    cos_tab = jnp.concatenate([cos_half, cos_half], axis=1)
    sin_tab = jnp.concatenate([-sin_half, sin_half], axis=1)

    query_grad, pair_grad, gathered, tok_pieces = gather_attend(
        old_place, weight_slots.reshape(slot_rows // BR, BR, width), tokens,
        queries.reshape(tok_count, -1), out_grad.reshape(tok_count, -1), segment_ids,
        cos_tab, sin_tab, head_count, dp_count,
    )
    gathered = gathered.reshape(2 * head_count, block_count * BR, head_size)

    slot_ids = jnp.arange(slot_total, dtype=jnp.int32)
    matched = (new_place[None, :] == slot_ids[:, None]).astype(jnp.int32)
    block_of = jnp.sum(matched * jnp.arange(block_count, dtype=jnp.int32)[None, :], axis=1)
    used = jnp.sum(matched, axis=1)
    me = lax.axis_index("mp")
    share = block_count // mp_count
    total = None
    for gap in range(1, mp_count):
        target = lax.rem(me + gap, mp_count)
        piece = input_part(pair_grad, gathered, target, share)
        ring = [(i, (i + gap) % mp_count) for i in range(mp_count)]
        arrived = lax.ppermute(piece, "mp", ring)
        total = arrived if total is None else total + arrived
    weight_grad = scatter_sum(tok_pieces, pair_grad, block_of, used, dp_count)
    input_grad = input_part(pair_grad, gathered, me, share, total)
    return (
        input_grad,
        query_grad.reshape(queries.shape),
        weight_grad.reshape(slot_rows, head_count, 2, head_size),
    )


def solution(mesh):
    return jax.shard_map(
        local,
        mesh=mesh,
        in_specs=(
            P("dp", None),
            P("dp", "mp", None),
            P("dp", "mp", None),
            P("dp", None),
            P("dp", "mp", None, None),
            P(),
            P(),
        ),
        out_specs=(P("dp", "mp"), P("dp", "mp", None), P("dp", "mp", None, None)),
        check_vma=False,
    )
```

```python
import functools

import jax
import jax.numpy as jnp
import numpy as np
from jax import lax
from jax.experimental import pallas as pl
from jax.experimental.pallas import tpu as pltpu
from jax.sharding import PartitionSpec as P

BR = 128
LOG2E = 1.4426950408889634
VMEM_LIMIT = 60 * 1024 * 1024
MESH = pl.DeviceIdType.MESH


def group_of(count):
    for size in (8, 4, 2):
        if count % size == 0:
            return size
    return 1


def chip_at(chips, position):
    return jnp.where(position < chips // 2, 2 * position, 2 * (chips - 1 - position) + 1)


def position_of(chips, chip):
    return jnp.where(lax.rem(chip, 2) == 0, chip // 2, chips - 1 - chip // 2)


def meet(*sizes):
    barrier = pltpu.get_barrier_semaphore()
    for axis, count in sizes:
        me = lax.axis_index(axis)

        @pl.loop(1, count)
        def _(k):
            pl.semaphore_signal(
                barrier, inc=1, device_id={axis: lax.rem(me + k, count)}, device_id_type=MESH
            )

    pl.semaphore_wait(barrier, sum(count - 1 for _, count in sizes))


def remote(src, dst, sent, got, peer, axis="dp"):
    return pltpu.make_async_remote_copy(
        src_ref=src, dst_ref=dst, send_sem=sent, recv_sem=got,
        device_id={axis: peer}, device_id_type=MESH,
    )


def gather_kernel(
    chips, heads, subs, tile, place, slots_ref, tok_hbm, q_hbm, og_hbm, row_ref,
    freq_ref, dq_ref, pair_ref, w_hbm, tokt_hbm,
    tok, q_ref, og_ref, stage, tokt, w, got, total, kv, bias, key_t, rot_acc, val_acc,
    cos_ref, sin_ref, load_sem, stage_sem, save_sem, swap_sent, swap_got, ring_sent, ring_got, pass_sent, pass_got,
):
    dp_count = 2 * chips
    hops = chips // 2
    me = lax.axis_index("dp")
    core = lax.rem(me, 2)
    spot = position_of(chips, me // 2)
    partner = me + 1 - 2 * core
    groups, blocks, splits, rows, lane = w.shape
    per = chips // groups
    slots = slots_ref.shape[0]
    tok_count, hd = tok.shape[0], lane
    per_head = q_ref.shape[0] // heads
    near = (
        2 * chip_at(chips, lax.rem(spot + 1, chips)) + core,
        2 * chip_at(chips, lax.rem(spot + chips - 1, chips)) + core,
    )
    size = blocks // subs
    inv_root = 1.0 / (hd ** 0.5)

    load = pltpu.make_async_copy(tok_hbm, tok, load_sem)
    load.start()
    band = stage.shape[1]
    bands = tok_count // band

    def stage_copy(src, i, slot):
        return pltpu.make_async_copy(src.at[pl.ds(i * band, band)], stage.at[slot], stage_sem.at[slot])

    stage_copy(q_hbm, 0, 0).start()
    stage_copy(og_hbm, 0, 1).start()

    def part(position, owner):
        return position // per, lax.rem(position, per) * 2 + owner

    meet(("dp", dp_count))

    def swap_copy(k):
        peer = lax.rem(me + k, dp_count)
        group, split = part(position_of(chips, peer // 2), lax.rem(peer, 2))
        src = slots_ref.at[
            :, pl.ds(pl.multiple_of(split * rows, rows), rows),
            pl.ds(pl.multiple_of(group * lane, lane), lane),
        ]
        return remote(src, got.at[me], swap_sent.at[k], swap_got.at[k], peer)

    @pl.loop(1, dp_count)
    def _(k):
        swap_copy(k).start()

    my_group, my_split = part(spot, core)
    own_rows = pl.ds(pl.multiple_of(my_split * rows, rows), rows)
    own_lanes = pl.ds(pl.multiple_of(my_group * lane, lane), lane)
    got[me] = slots_ref[:, own_rows, own_lanes]

    kpos = lax.broadcasted_iota(jnp.int32, bias.shape, 0)
    qpos = lax.broadcasted_iota(jnp.int32, bias.shape, 1)
    ids = jnp.broadcast_to(row_ref[...].astype(jnp.float32), bias.shape)
    bias[...] = ids.T
    allowed = (kpos <= qpos) & (bias[...] == ids)
    bias[...] = jnp.where(allowed, 0.0, -1e30).astype(jnp.float32)
    spots = lax.broadcasted_iota(jnp.int32, cos_ref.shape, 0).astype(jnp.float32)
    lower = lax.broadcasted_iota(jnp.int32, cos_ref.shape, 1) < hd // 2
    angle = spots * freq_ref[...]
    cos_ref[...] = jnp.cos(angle)
    sine = jnp.sin(angle)
    sin_ref[...] = jnp.where(lower, -sine, sine)

    @pl.loop(0, bands)
    def _(i):
        at = pl.ds(pl.multiple_of(i * band, band), band)
        for slot, (src, dst) in enumerate(((q_hbm, q_ref), (og_hbm, og_ref))):
            stage_copy(src, i, slot).wait()
            dst[:, at, :] = pltpu.einshape("thd->htd", stage[slot])

            @pl.when(i + 1 < bands)
            def _():
                stage_copy(src, i + 1, slot).start()

    load.wait()

    @pl.loop(0, blocks)
    def _(b):
        cols = tok[:, pl.ds(pl.multiple_of(b * BR, BR), BR)]
        flipped = cols.astype(jnp.float32).T
        tokt[b] = flipped.reshape(splits, rows, tok_count).astype(jnp.bfloat16)

    save_tok = pltpu.make_async_copy(tokt, tokt_hbm, save_sem.at[groups])
    save_tok.start()

    @pl.loop(1, dp_count)
    def _(k):
        swap_copy(k).wait_recv()

    def piece(origin, owner, u):
        group, split = part(origin, owner)
        return w.at[group, pl.ds(u * size, size), split]

    def ring_copy(way, hop, u):
        origin = lax.rem(spot + hop if way else spot - hop + chips, chips)
        ref = piece(origin, core, u)
        peer = near[1] if way else near[0]
        return remote(ref, ref, ring_sent.at[way, hop - 1, u], ring_got.at[way, hop - 1, u], peer)

    def forward(way, hop, u):
        origin = lax.rem(spot + hop - 1 if way else spot - hop + 1 + chips, chips)
        ref = piece(origin, core, u)
        peer = near[1] if way else near[0]
        return remote(ref, ref, ring_sent.at[way, hop - 1, u], ring_got.at[way, hop - 1, u], peer)

    def pass_copy(origin, owner, u):
        ref = piece(origin, owner, u)
        return remote(ref, ref, pass_sent.at[origin, u], pass_got.at[origin, u], partner)

    def carried(way, hop, u):
        mine = (u < subs // 2) if way == 0 else (u >= subs // 2)
        return (hop < hops) | ((hop == hops) & mine)

    @pl.loop(0, subs)
    def _(u):
        for i in range(size):
            b = u * size + i
            slot = place[b]
            w[my_group, b, my_split] = got[slot // slots, lax.rem(slot, slots)]
        for way in range(2):
            @pl.when(carried(way, 1, u))
            def _():
                forward(way, 1, u).start()
        pass_copy(spot, core, u).start()

    def receive(hop, u):
        for way in range(2):
            @pl.when(carried(way, hop, u))
            def _():
                ring_copy(way, hop, u).wait_recv()
                origin = lax.rem(spot + hop if way else spot - hop + chips, chips)
                pass_copy(origin, core, u).start()

                @pl.when((hop < hops) & carried(way, hop + 1, u))
                def _():
                    forward(way, hop + 1, u).start()

    def shared(origin):
        @pl.loop(0, subs)
        def _(u):
            pass_copy(origin, 1 - core, u).wait_recv()

    def save_copy(group):
        return pltpu.make_async_copy(w.at[group], w_hbm.at[group], save_sem.at[group])

    def begin(head):
        for g in range(2):
            save_copy(2 * head + g).start()
        total[...] = jnp.zeros_like(total)
        step = group_of(blocks)

        @pl.loop(0, blocks // step)
        def _(i):
            ws = [
                w[2 * head + g, pl.ds(i * step, step)].reshape(step * splits * rows, lane)
                for g in range(2)
            ]
            cols = pl.ds(pl.multiple_of(i * step * BR, step * BR), step * BR)
            total[...] += jnp.dot(
                tok[:, cols], jnp.concatenate(ws, axis=1), preferred_element_type=jnp.float32
            )

        key = total[:, :hd]
        rot = key * cos_ref[...] + pltpu.roll(key, hd // 2, 1) * sin_ref[...]
        rot = rot.astype(jnp.bfloat16)
        kv[:, :hd] = rot
        kv[:, hd:] = total[:, hd:].astype(jnp.bfloat16)
        key_t[...] = rot.astype(jnp.float32).T.astype(jnp.bfloat16)
        rot_acc[...] = jnp.zeros_like(rot_acc)
        val_acc[...] = jnp.zeros_like(val_acc)

    def unit(head, t):
        span = slice(t * tile, (t + 1) * tile)
        lo, reach = max(0, t * tile - tok_count // 2), (t + 1) * tile
        stack = pl.ds(head * per_head, per_head)
        q = q_ref[stack, span, :].reshape(per_head * tile, hd)
        og = og_ref[stack, span, :].reshape(per_head * tile, hd)
        nt = (((1,), (1,)), ((), ()))
        s = lax.dot_general(kv[lo:reach, :hd], q, nt, preferred_element_type=jnp.float32)
        s = s * (inv_root * LOG2E) + jnp.concatenate([bias[lo:reach, span]] * per_head, axis=1)
        e = jnp.exp2(s - jnp.max(s, axis=0, keepdims=True))
        p = e * (1.0 / jnp.sum(e, axis=0, keepdims=True))
        pb = p.astype(jnp.bfloat16)
        dp = lax.dot_general(kv[lo:reach, hd:], og, nt, preferred_element_type=jnp.float32)
        dot = jnp.sum(pb.astype(jnp.float32) * dp, axis=0, keepdims=True)
        ds = (p * (dp - dot)).astype(jnp.bfloat16)
        val_acc[lo:reach, :] += jnp.dot(pb, og, preferred_element_type=jnp.float32)
        rot_acc[lo:reach, :] += jnp.dot(ds, q, preferred_element_type=jnp.float32)
        dq = jnp.dot(key_t[:, lo:reach], ds, preferred_element_type=jnp.float32)
        dq = (dq * inv_root).T.astype(jnp.bfloat16).reshape(per_head, tile, hd)
        dq_ref[span, pl.ds(pl.multiple_of(head * per_head, per_head), per_head), :] = (
            pltpu.einshape("htd->thd", dq)
        )

    def finish(head):
        g = rot_acc[...] * inv_root
        back = g * cos_ref[...] - pltpu.roll(g, hd // 2, 1) * sin_ref[...]
        at = pl.multiple_of(head * 2 * hd, 2 * hd)
        pair_ref[:, pl.ds(at, hd)] = back.astype(jnp.bfloat16)
        pair_ref[:, pl.ds(at + hd, hd)] = val_acc[...].astype(jnp.bfloat16)

    tiles = tok_count // tile
    if groups == chips and heads == hops and subs % tiles == 0:
        def head_at(k):
            side = jnp.where(lax.rem(k + spot, 2) == 0, 1, -1)
            return lax.rem(spot // 2 + side * ((k + 1) // 2) + 2 * heads, heads)

        @pl.loop(0, hops + 1)
        def _(t):
            head = head_at(jnp.maximum(t - 1, 0))

            @pl.when(t >= 1)
            def _():
                shared(2 * head)
                shared(2 * head + 1)
                begin(head)

            for i in range(tiles):
                @pl.when(t < hops)
                def _():
                    @pl.loop(i * (subs // tiles), (i + 1) * (subs // tiles))
                    def _(u):
                        receive(t + 1, u)

                @pl.when(t >= 1)
                def _():
                    unit(head, i)

            @pl.when(t >= 1)
            def _():
                finish(head)
    else:
        @pl.loop(0, hops)
        def _(t):
            @pl.loop(0, subs)
            def _(u):
                receive(t + 1, u)

        @pl.loop(0, chips)
        def _(origin):
            shared(origin)

        @pl.loop(0, heads)
        def _(head):
            begin(head)

            for i in range(tiles):
                unit(head, i)

            finish(head)

    @pl.loop(1, dp_count)
    def _(k):
        swap_copy(k).wait_send()

    @pl.loop(0, subs)
    def _(u):
        @pl.loop(0, chips)
        def _(origin):
            pass_copy(origin, core, u).wait_send()

        @pl.loop(1, hops + 1)
        def _(hop):
            for way in range(2):
                @pl.when(carried(way, hop, u))
                def _():
                    forward(way, hop, u).wait_send()

    @pl.loop(0, groups)
    def _(group):
        save_copy(group).wait()

    save_tok.wait()


def gather_attend(place, slots, tokens, queries, out_grad, seg_row, head_count, dp_count):
    slot_count, _, width = slots.shape
    tok_count = queries.shape[0]
    q_width = queries.shape[1] * queries.shape[2]
    chips = dp_count // 2
    lane = width // head_count // 2
    groups = 2 * head_count
    blocks = place.shape[0]
    splits = dp_count // groups
    rows = BR // splits
    subs = 8
    hops = chips // 2
    tile = 128
    powers = np.power(500000.0, -2.0 * np.arange(lane // 2) / lane)
    frequency = np.concatenate([powers, powers]).astype(np.float32)[None, :]
    turned = (queries.shape[1], tok_count, lane)
    bf = jnp.bfloat16
    f32 = jnp.float32
    whole = pl.BlockSpec(memory_space=pltpu.VMEM)
    far = pl.BlockSpec(memory_space=pl.ANY)
    dma = pltpu.SemaphoreType.DMA
    return pl.pallas_call(
        functools.partial(gather_kernel, chips, head_count, subs, tile),
        out_shape=(
            jax.ShapeDtypeStruct(queries.shape, bf),
            jax.ShapeDtypeStruct((tok_count, width), bf),
            jax.ShapeDtypeStruct((groups, blocks, splits, rows, lane), bf),
            jax.ShapeDtypeStruct((blocks, splits, rows, tok_count), bf),
        ),
        in_specs=[pl.BlockSpec(memory_space=pltpu.SMEM), whole, far, far, far, whole, whole],
        out_specs=(whole, whole, far, far),
        scratch_shapes=[
            pltpu.VMEM(tokens.shape, bf),
            pltpu.VMEM(turned, bf),
            pltpu.VMEM(turned, bf),
            pltpu.VMEM((2, tile) + queries.shape[1:], bf),
            pltpu.VMEM((blocks, splits, rows, tok_count), bf),
            pltpu.VMEM((groups, blocks, splits, rows, lane), bf),
            pltpu.VMEM((dp_count, slot_count, rows, lane), bf),
            pltpu.VMEM((tok_count, 2 * lane), f32),
            pltpu.VMEM((tok_count, 2 * lane), bf),
            pltpu.VMEM((tok_count, tok_count), f32),
            pltpu.VMEM((lane, tok_count), bf),
            pltpu.VMEM((tok_count, lane), f32),
            pltpu.VMEM((tok_count, lane), f32),
            pltpu.VMEM((tok_count, lane), f32),
            pltpu.VMEM((tok_count, lane), f32),
            dma,
            dma((2,)),
            dma((groups + 1,)),
            dma((dp_count,)),
            dma((dp_count,)),
            dma((2, hops, subs)),
            dma((2, hops, subs)),
            dma((chips, subs)),
            dma((chips, subs)),
        ],
        compiler_params=pltpu.CompilerParams(
            collective_id=1, has_side_effects=True, vmem_limit_bytes=VMEM_LIMIT
        ),
        cost_estimate=pl.CostEstimate(
            flops=10 * tok_count * tok_count * q_width, bytes_accessed=10**8,
            transcendentals=tok_count * tok_count * q_width // lane,
        ),
        name="gather_attend",
    )(place, slots, tokens, queries, out_grad, seg_row, frequency)


def scatter_kernel(
    chips, mp_count, subs, block_of, used, tok_hbm, pair_ref, w_hbm, out_ref, in_ref, tok_ref,
    part_out, part_in, ring_out, ring_in, ready, final, swap_out, swap_in, wbuf, side_out, side_in,
    part_sent, part_got, ring_sent, ring_got, swap_sent, swap_got, tok_sem, load_sem, side_sent, side_got,
):
    dp_count = 2 * chips
    me, my = lax.axis_index("dp"), lax.axis_index("mp")
    core = lax.rem(me, 2)
    spot = position_of(chips, me // 2)
    ahead = 2 * chip_at(chips, lax.rem(spot + 1, chips)) + core
    behind = 2 * chip_at(chips, lax.rem(spot + chips - 1, chips)) + core
    partner = me + 1 - 2 * core
    blocks, splits, rows, tok_count = tok_ref.shape
    lane = final.shape[2]
    groups = pair_ref.shape[1] // lane
    per = chips // groups
    half = blocks // 2
    size = half // subs
    slots = swap_out.shape[1]
    keep, early = part_out.shape[1], part_out.shape[1] - 1
    deep = wbuf.shape[2]
    features = in_ref.shape[1]
    chunks = features // deep
    others, units = (mp_count - 1) * chunks, mp_count * chunks

    def load_copy(k):
        target = lax.rem(my + 1 + k // chunks, mp_count)
        start = pl.multiple_of(target * features + lax.rem(k, chunks) * deep, deep)
        slot = lax.rem(k, 2)
        return pltpu.make_async_copy(
            w_hbm.at[:, pl.ds(start, deep), :], wbuf.at[slot], load_sem.at[slot]
        )

    loads = [
        pltpu.make_async_copy(
            tok_hbm.at[pl.ds(i * half, half)], tok_ref.at[pl.ds(i * half, half)], tok_sem.at[i]
        )
        for i in range(2)
    ]
    for load in loads:
        load.start()
    load_copy(0).start()
    meet(("dp", dp_count), ("mp", mp_count))

    def goal(way, step):
        return lax.rem(spot + (chips - 1 - step if way == 0 else 1 + step), chips)

    def product(way, step, owner, u):
        position = goal(way, step)
        split = lax.rem(position, per) * 2 + owner
        left = tok_ref[way * half + u * size : way * half + (u + 1) * size, split]
        lanes = pl.ds(pl.multiple_of((position // per) * lane, lane), lane)
        return jnp.dot(
            left.reshape(size * rows, tok_count), pair_ref[:, lanes],
            preferred_element_type=jnp.float32,
        ).reshape(size, rows, lane)

    def part_copy(way, step):
        return remote(
            part_out.at[way, lax.rem(step, keep)], part_in.at[way, step],
            part_sent.at[way, step], part_got.at[way, step], partner,
        )

    def ring_copy(way, step, u):
        at = pl.ds(u * size, size)
        return remote(
            ring_out.at[way, lax.rem(step, 2), at], ring_in.at[way, step, at],
            ring_sent.at[way, step, u], ring_got.at[way, step, u],
            ahead if way == 0 else behind,
        )

    def span(u):
        return slice(u * size, (u + 1) * size)

    def part_fill(step, way, u):
        part_out[way, lax.rem(step, keep), span(u)] = product(way, step, 1 - core, u).astype(
            jnp.bfloat16
        )

    def ready_fill(step, way, u):
        ready[way, span(u)] = product(way, step, core, u) + part_in[way, step, span(u)].astype(
            jnp.float32
        )

    def ring_step(step, last):
        if not last:
            for way in range(2):
                part_copy(way, step + 1).wait_recv()

            @pl.when(step + early < chips)
            def _():
                for way in range(2):
                    part_copy(way, step - 1).wait_send()

        for u in range(subs):
            for way in range(2):
                ring_copy(way, step - 1, u).wait_recv()
                total = ready[way, span(u)] + ring_in[way, step - 1, span(u)].astype(jnp.float32)
                if last:
                    final[way * half + u * size : way * half + (u + 1) * size] = total.astype(
                        jnp.bfloat16
                    )
                else:
                    @pl.when(step >= 2)
                    def _():
                        ring_copy(way, step - 2, u).wait_send()

                    ring_out[way, lax.rem(step, 2), span(u)] = total.astype(jnp.bfloat16)
                    ring_copy(way, step, u).start()
                    ready_fill(step + 1, way, u)

                    @pl.when(step + early < chips)
                    def _():
                        part_fill(step + early, way, u)
        if not last:
            @pl.when(step + early < chips)
            def _():
                for way in range(2):
                    part_copy(way, step + early).start()

    def side_copy(k):
        target = lax.rem(my + 1 + k // chunks, mp_count)
        return remote(
            side_out.at[k], side_in.at[k], side_sent.at[k], side_got.at[k], target, "mp"
        )

    def unit(k):
        load_copy(k).wait()

        @pl.when(k + 1 < units)
        def _():
            load_copy(k + 1).start()

        slot = lax.rem(k, 2)
        w = jnp.concatenate([wbuf[slot, g] for g in range(groups)], axis=1)
        value = lax.dot_general(
            pair_ref[...], w, (((1,), (1,)), ((), ())), preferred_element_type=jnp.float32
        )

        @pl.when(k < others)
        def _():
            side_out[k] = value.astype(jnp.bfloat16)
            side_copy(k).start()

        @pl.when(k >= others)
        def _():
            chunk = k - others
            total = value
            for gap in range(mp_count - 1):
                side_copy(gap * chunks + chunk).wait_recv()
                total = total + side_in[gap * chunks + chunk].astype(jnp.float32)
            in_ref[:, pl.ds(pl.multiple_of(chunk * deep, deep), deep)] = total.astype(jnp.bfloat16)

    for load in loads:
        load.wait()
    for way in range(2):
        for u in range(subs):
            part_fill(0, way, u)
        part_copy(way, 0).start()
    for way in range(2):
        for u in range(subs):
            ready[way, span(u)] = product(way, 0, core, u)
    for way in range(2):
        part_copy(way, 0).wait_recv()
    for u in range(subs):
        for way in range(2):
            total = ready[way, span(u)] + part_in[way, 0, span(u)].astype(jnp.float32)
            ring_out[way, 0, span(u)] = total.astype(jnp.bfloat16)
            ring_copy(way, 0, u).start()
    for step in range(1, early + 1):
        for way in range(2):
            for u in range(subs):
                part_fill(step, way, u)
            part_copy(way, step).start()
    for way in range(2):
        part_copy(way, 1).wait_recv()
        for u in range(subs):
            ready_fill(1, way, u)
    pace = 2

    @pl.loop(1, chips - 1)
    def _(step):
        ring_step(step, False)

        @pl.loop((step - 1) * pace, step * pace)
        def _(k):
            @pl.when(k < units)
            def _():
                unit(k)

    ring_step(chips - 1, True)

    def swap_copy(k):
        peer = lax.rem(me + k, dp_count)
        return remote(swap_out.at[peer], swap_in.at[me], swap_sent.at[k], swap_got.at[k], peer)

    def fill(peer):
        for i in range(slots):
            slot = peer * slots + i
            taken = final[block_of[slot]]
            swap_out[peer, i] = jnp.where(used[slot] != 0, taken, jnp.zeros_like(taken))

    def place_in(origin, value):
        position = position_of(chips, origin // 2)
        split = lax.rem(position, per) * 2 + lax.rem(origin, 2)
        for i in range(slots):
            start = (i * BR + split * rows) * groups + position // per
            out_ref[pl.ds(start, rows, stride=groups), :] = value[i].astype(jnp.float32)

    @pl.loop(1, dp_count)
    def _(k):
        fill(lax.rem(me + k, dp_count))
        swap_copy(k).start()

    fill(me)
    place_in(me, swap_out[me])

    @pl.loop(min((chips - 2) * pace, units), units)
    def _(k):
        unit(k)

    @pl.loop(1, dp_count)
    def _(k):
        swap_copy(k).wait_recv()
        origin = lax.rem(me + dp_count - k, dp_count)
        place_in(origin, swap_in[origin])

    @pl.loop(1, dp_count)
    def _(k):
        swap_copy(k).wait_send()

    @pl.loop(0, others)
    def _(k):
        side_copy(k).wait_send()

    @pl.loop(max(chips - keep, 0), chips)
    def _(step):
        for way in range(2):
            part_copy(way, step).wait_send()

    @pl.loop(max(chips - 3, 0), chips - 1)
    def _(step):
        for way in range(2):
            for u in range(subs):
                ring_copy(way, step, u).wait_send()


def scatter_sum(tok_pieces, pairs, gathered, block_of, used, dp_count, mp_count):
    chips = dp_count // 2
    width = pairs.shape[1]
    blocks, splits, rows, tok_count = tok_pieces.shape
    groups, lane = gathered.shape[0], gathered.shape[2]
    slots = block_of.shape[0] // dp_count
    subs = 4
    keep = 4
    whole = pl.BlockSpec(memory_space=pltpu.VMEM)
    scalars = pl.BlockSpec(memory_space=pltpu.SMEM)
    far = pl.BlockSpec(memory_space=pl.ANY)
    half = blocks // 2
    features = blocks * BR // mp_count
    deep = group_of(features // BR) // 2 * BR
    others = (mp_count - 1) * features // deep
    bf = jnp.bfloat16
    dma = pltpu.SemaphoreType.DMA
    return pl.pallas_call(
        functools.partial(scatter_kernel, chips, mp_count, subs),
        out_shape=(
            jax.ShapeDtypeStruct((slots * BR * groups, lane), jnp.float32),
            jax.ShapeDtypeStruct((tok_count, features), bf),
        ),
        in_specs=[scalars, scalars, far, whole, far],
        out_specs=(whole, whole),
        scratch_shapes=[
            pltpu.VMEM(tok_pieces.shape, bf),
            pltpu.VMEM((2, keep, half, rows, lane), bf),
            pltpu.VMEM((2, chips, half, rows, lane), bf),
            pltpu.VMEM((2, 2, half, rows, lane), bf),
            pltpu.VMEM((2, chips - 1, half, rows, lane), bf),
            pltpu.VMEM((2, half, rows, lane), jnp.float32),
            pltpu.VMEM((blocks, rows, lane), bf),
            pltpu.VMEM((dp_count, slots, rows, lane), bf),
            pltpu.VMEM((dp_count, slots, rows, lane), bf),
            pltpu.VMEM((2, groups, deep, lane), bf),
            pltpu.VMEM((others, tok_count, deep), bf),
            pltpu.VMEM((others, tok_count, deep), bf),
            dma((2, chips)),
            dma((2, chips)),
            dma((2, chips - 1, subs)),
            dma((2, chips - 1, subs)),
            dma((dp_count,)),
            dma((dp_count,)),
            dma((2,)),
            dma((2,)),
            dma((others,)),
            dma((others,)),
        ],
        compiler_params=pltpu.CompilerParams(
            collective_id=0, has_side_effects=True, vmem_limit_bytes=VMEM_LIMIT
        ),
        cost_estimate=pl.CostEstimate(
            flops=16 * tok_pieces.size * width, bytes_accessed=10**8, transcendentals=0
        ),
        name="scatter_sum",
    )(block_of, used, tok_pieces, pairs, gathered)


def local(tokens, queries, out_grad, segment_ids, weight_slots, old_place, new_place):
    tok_count = tokens.shape[0]
    slot_rows, head_count, _, head_size = weight_slots.shape
    width = head_count * 2 * head_size
    dp_count = lax.axis_size("dp")
    mp_count = lax.axis_size("mp")
    slot_total = dp_count * (slot_rows // BR)
    block_count = old_place.shape[0]

    query_grad, pair_grad, gathered, tok_pieces = gather_attend(
        old_place, weight_slots.reshape(slot_rows // BR, BR, width), tokens,
        queries, out_grad, segment_ids, head_count, dp_count,
    )
    gathered = gathered.reshape(2 * head_count, block_count * BR, head_size)

    slot_ids = jnp.arange(slot_total, dtype=jnp.int32)
    matched = (new_place[None, :] == slot_ids[:, None]).astype(jnp.int32)
    block_of = jnp.sum(matched * jnp.arange(block_count, dtype=jnp.int32)[None, :], axis=1)
    used = jnp.sum(matched, axis=1)
    weight_grad, input_grad = scatter_sum(
        tok_pieces, pair_grad, gathered, block_of, used, dp_count, mp_count
    )
    return (
        input_grad,
        query_grad,
        weight_grad.reshape(slot_rows, head_count, 2, head_size),
    )


def solution(mesh):
    return jax.shard_map(
        local,
        mesh=mesh,
        in_specs=(
            P("dp", None),
            P("dp", "mp", None),
            P("dp", "mp", None),
            P("dp", None),
            P("dp", "mp", None, None),
            P(),
            P(),
        ),
        out_specs=(P("dp", "mp"), P("dp", "mp", None), P("dp", "mp", None, None)),
        check_vma=False,
    )
```

```python
import functools

import jax
import jax.numpy as jnp
import numpy as np
from jax import lax
from jax.experimental import pallas as pl
from jax.experimental.pallas import tpu as pltpu
from jax.sharding import PartitionSpec as P

BR = 128
LOG2E = 1.4426950408889634
VMEM_LIMIT = 63 * 1024 * 1024
MESH = pl.DeviceIdType.MESH


def group_of(count):
    for size in (8, 4, 2):
        if count % size == 0:
            return size
    return 1


def chip_at(chips, position):
    return jnp.where(position < chips // 2, 2 * position, 2 * (chips - 1 - position) + 1)


def position_of(chips, chip):
    return jnp.where(lax.rem(chip, 2) == 0, chip // 2, chips - 1 - chip // 2)


def meet(*sizes):
    barrier = pltpu.get_barrier_semaphore()
    for axis, count in sizes:
        me = lax.axis_index(axis)

        @pl.loop(1, count)
        def _(k):
            pl.semaphore_signal(
                barrier, inc=1, device_id={axis: lax.rem(me + k, count)}, device_id_type=MESH
            )

    pl.semaphore_wait(barrier, sum(count - 1 for _, count in sizes))


def remote(src, dst, sent, got, peer, axis="dp"):
    return pltpu.make_async_remote_copy(
        src_ref=src, dst_ref=dst, send_sem=sent, recv_sem=got,
        device_id={axis: peer}, device_id_type=MESH,
    )


def gather_kernel(
    chips, heads, subs, tile, place, native, tok_hbm, q_hbm, og_hbm, row_ref,
    freq_ref, dq_ref, pair_ref, w_hbm, tokt_hbm, first_hbm,
    tok, q_ref, og_ref, stage, tokt, w, got, total, kv, bias, key_t, rot_acc, val_acc,
    cos_ref, sin_ref, load_sem, stage_sem, save_sem, swap_sent, swap_got, ring_sent, ring_got, pass_sent, pass_got,
    near_out, near_in, first_out, first_in, near_sent, near_got, first_sent, first_got, slots_ref,
):
    dp_count = 2 * chips
    hops = chips // 2
    me = lax.axis_index("dp")
    core = lax.rem(me, 2)
    spot = position_of(chips, me // 2)
    partner = me + 1 - 2 * core
    groups, blocks, splits, rows, lane = w.shape
    per = chips // groups
    slots = slots_ref.shape[0]
    tok_count, hd = tok.shape[0], lane
    per_head = q_ref.shape[0] // heads
    near = (
        2 * chip_at(chips, lax.rem(spot + 1, chips)) + core,
        2 * chip_at(chips, lax.rem(spot + chips - 1, chips)) + core,
    )
    size = blocks // subs
    inv_root = 1.0 / (hd ** 0.5)

    load = pltpu.make_async_copy(tok_hbm, tok, load_sem)
    load.start()
    band = stage.shape[1]
    bands = tok_count // band

    def stage_copy(src, i, slot):
        return pltpu.make_async_copy(src.at[pl.ds(i * band, band)], stage.at[slot], stage_sem.at[slot])

    stage_copy(q_hbm, 0, 0).start()
    stage_copy(og_hbm, 0, 1).start()

    for i in range(slots):
        turned = pltpu.einshape("rgd->grd", native[i])
        for g in range(groups):
            slots_ref[i, :, g * lane : (g + 1) * lane] = turned[g]

    def part(position, owner):
        return position // per, lax.rem(position, per) * 2 + owner

    meet(("dp", dp_count))

    def swap_copy(k):
        peer = lax.rem(me + k, dp_count)
        group, split = part(position_of(chips, peer // 2), lax.rem(peer, 2))
        src = slots_ref.at[
            :, pl.ds(pl.multiple_of(split * rows, rows), rows),
            pl.ds(pl.multiple_of(group * lane, lane), lane),
        ]
        return remote(src, got.at[me], swap_sent.at[k], swap_got.at[k], peer)

    @pl.loop(1, dp_count)
    def _(k):
        swap_copy(k).start()

    my_group, my_split = part(spot, core)
    own_rows = pl.ds(pl.multiple_of(my_split * rows, rows), rows)
    own_lanes = pl.ds(pl.multiple_of(my_group * lane, lane), lane)
    got[me] = slots_ref[:, own_rows, own_lanes]

    kpos = lax.broadcasted_iota(jnp.int32, bias.shape, 0)
    qpos = lax.broadcasted_iota(jnp.int32, bias.shape, 1)
    ids = jnp.broadcast_to(row_ref[...].astype(jnp.float32), bias.shape)
    bias[...] = ids.T
    allowed = (kpos <= qpos) & (bias[...] == ids)
    bias[...] = jnp.where(allowed, 0.0, -1e30).astype(jnp.float32)
    spots = lax.broadcasted_iota(jnp.int32, cos_ref.shape, 0).astype(jnp.float32)
    lower = lax.broadcasted_iota(jnp.int32, cos_ref.shape, 1) < hd // 2
    angle = spots * freq_ref[...]
    cos_ref[...] = jnp.cos(angle)
    sine = jnp.sin(angle)
    sin_ref[...] = jnp.where(lower, -sine, sine)

    @pl.loop(0, bands)
    def _(i):
        at = pl.ds(pl.multiple_of(i * band, band), band)
        for slot, (src, dst) in enumerate(((q_hbm, q_ref), (og_hbm, og_ref))):
            stage_copy(src, i, slot).wait()
            dst[:, at, :] = pltpu.einshape("thd->htd", stage[slot])

            @pl.when(i + 1 < bands)
            def _():
                stage_copy(src, i + 1, slot).start()

    load.wait()

    @pl.loop(0, blocks)
    def _(b):
        cols = tok[:, pl.ds(pl.multiple_of(b * BR, BR), BR)]
        flipped = cols.astype(jnp.float32).T
        tokt[b] = flipped.reshape(splits, rows, tok_count).astype(jnp.bfloat16)

    save_tok = pltpu.make_async_copy(tokt, tokt_hbm, save_sem.at[groups])
    save_tok.start()

    @pl.loop(1, dp_count)
    def _(k):
        swap_copy(k).wait_recv()

    def piece(origin, owner, u):
        group, split = part(origin, owner)
        return w.at[group, pl.ds(u * size, size), split]

    def ring_copy(way, hop, u):
        origin = lax.rem(spot + hop if way else spot - hop + chips, chips)
        ref = piece(origin, core, u)
        peer = near[1] if way else near[0]
        return remote(ref, ref, ring_sent.at[way, hop - 1, u], ring_got.at[way, hop - 1, u], peer)

    def forward(way, hop, u):
        origin = lax.rem(spot + hop - 1 if way else spot - hop + 1 + chips, chips)
        ref = piece(origin, core, u)
        peer = near[1] if way else near[0]
        return remote(ref, ref, ring_sent.at[way, hop - 1, u], ring_got.at[way, hop - 1, u], peer)

    def pass_copy(origin, owner, u):
        ref = piece(origin, owner, u)
        return remote(ref, ref, pass_sent.at[origin, u], pass_got.at[origin, u], partner)

    def carried(way, hop, u):
        mine = (u < subs // 2) if way == 0 else (u >= subs // 2)
        return (hop < hops) | ((hop == hops) & mine)

    @pl.loop(0, subs)
    def _(u):
        for i in range(size):
            b = u * size + i
            slot = place[b]
            w[my_group, b, my_split] = got[slot // slots, lax.rem(slot, slots)]
        for way in range(2):
            @pl.when(carried(way, 1, u))
            def _():
                forward(way, 1, u).start()
        pass_copy(spot, core, u).start()

    def receive(hop, u):
        for way in range(2):
            @pl.when(carried(way, hop, u))
            def _():
                ring_copy(way, hop, u).wait_recv()
                origin = lax.rem(spot + hop if way else spot - hop + chips, chips)
                pass_copy(origin, core, u).start()

                @pl.when((hop < hops) & carried(way, hop + 1, u))
                def _():
                    forward(way, hop + 1, u).start()

    def shared(origin):
        @pl.loop(0, subs)
        def _(u):
            pass_copy(origin, 1 - core, u).wait_recv()

    def save_copy(group):
        return pltpu.make_async_copy(w.at[group], w_hbm.at[group], save_sem.at[group])

    def begin(head):
        for g in range(2):
            save_copy(2 * head + g).start()
        total[...] = jnp.zeros_like(total)
        step = group_of(blocks)

        @pl.loop(0, blocks // step)
        def _(i):
            ws = [
                w[2 * head + g, pl.ds(i * step, step)].reshape(step * splits * rows, lane)
                for g in range(2)
            ]
            cols = pl.ds(pl.multiple_of(i * step * BR, step * BR), step * BR)
            total[...] += jnp.dot(
                tok[:, cols], jnp.concatenate(ws, axis=1), preferred_element_type=jnp.float32
            )

        key = total[:, :hd]
        rot = key * cos_ref[...] + pltpu.roll(key, hd // 2, 1) * sin_ref[...]
        rot = rot.astype(jnp.bfloat16)
        kv[:, :hd] = rot
        kv[:, hd:] = total[:, hd:].astype(jnp.bfloat16)
        key_t[...] = rot.astype(jnp.float32).T.astype(jnp.bfloat16)
        rot_acc[...] = jnp.zeros_like(rot_acc)
        val_acc[...] = jnp.zeros_like(val_acc)

    def unit(head, t):
        span = slice(t * tile, (t + 1) * tile)
        lo, reach = max(0, t * tile - tok_count // 2), (t + 1) * tile
        stack = pl.ds(head * per_head, per_head)
        q = q_ref[stack, span, :].reshape(per_head * tile, hd)
        og = og_ref[stack, span, :].reshape(per_head * tile, hd)
        nt = (((1,), (1,)), ((), ()))
        s = lax.dot_general(kv[lo:reach, :hd], q, nt, preferred_element_type=jnp.float32)
        s = s * (inv_root * LOG2E) + jnp.concatenate([bias[lo:reach, span]] * per_head, axis=1)
        e = jnp.exp2(s - jnp.max(s, axis=0, keepdims=True))
        p = e * (1.0 / jnp.sum(e, axis=0, keepdims=True))
        pb = p.astype(jnp.bfloat16)
        dp = lax.dot_general(kv[lo:reach, hd:], og, nt, preferred_element_type=jnp.float32)
        dot = jnp.sum(pb.astype(jnp.float32) * dp, axis=0, keepdims=True)
        ds = (p * (dp - dot)).astype(jnp.bfloat16)
        val_acc[lo:reach, :] += jnp.dot(pb, og, preferred_element_type=jnp.float32)
        rot_acc[lo:reach, :] += jnp.dot(ds, q, preferred_element_type=jnp.float32)
        dq = jnp.dot(key_t[:, lo:reach], ds, preferred_element_type=jnp.float32)
        dq = (dq * inv_root).T.astype(jnp.bfloat16).reshape(per_head, tile, hd)
        dq_ref[span, pl.ds(pl.multiple_of(head * per_head, per_head), per_head), :] = (
            pltpu.einshape("htd->thd", dq)
        )

    def finish(head):
        g = rot_acc[...] * inv_root
        back = g * cos_ref[...] - pltpu.roll(g, hd // 2, 1) * sin_ref[...]
        at = pl.multiple_of(head * 2 * hd, 2 * hd)
        pair_ref[:, pl.ds(at, hd)] = back.astype(jnp.bfloat16)
        pair_ref[:, pl.ds(at + hd, hd)] = val_acc[...].astype(jnp.bfloat16)

    half = blocks // 2
    quarter = half // 4

    def near_copy(way):
        return remote(
            near_out.at[way], near_in.at[way], near_sent.at[way], near_got.at[way], partner
        )

    def first_copy(way):
        peer = jnp.where(way == 0, near[0], near[1])
        return remote(
            first_out.at[way], first_in.at[way], first_sent.at[way], first_got.at[way], peer
        )

    def first_part(way):
        goal = lax.rem(jnp.where(way == 0, spot + chips - 1, spot + 1), chips)

        def product(u, owner):
            group, split = part(goal, owner)
            left = tokt[pl.ds(way * half + u * quarter, quarter), split]
            lanes = pl.ds(pl.multiple_of(group * lane, lane), lane)
            return jnp.dot(
                left.reshape(quarter * rows, tok_count), pair_ref[:, lanes],
                preferred_element_type=jnp.float32,
            ).reshape(quarter, rows, lane)

        for u in range(4):
            at = slice(u * quarter, (u + 1) * quarter)
            near_out[way, at] = product(u, 1 - core).astype(jnp.bfloat16)
        near_copy(way).start()
        for u in range(4):
            at = slice(u * quarter, (u + 1) * quarter)
            mine = product(u, core)
            if u == 0:
                near_copy(way).wait_recv()
            first_out[way, at] = (mine + near_in[way, at].astype(jnp.float32)).astype(jnp.bfloat16)

    tiles = tok_count // tile
    if groups == chips and heads == hops >= 4 and subs % tiles == 0:
        def head_at(k):
            side = jnp.where(lax.rem(k + spot, 2) == 0, 1, -1)
            return lax.rem(spot // 2 + side * ((k + 1) // 2) + 2 * heads, heads)

        @pl.loop(0, hops + 1)
        def _(t):
            head = head_at(jnp.maximum(t - 1, 0))

            @pl.when(t >= 1)
            def _():
                shared(2 * head)
                shared(2 * head + 1)
                begin(head)

            for i in range(tiles):
                @pl.when(t < hops)
                def _():
                    @pl.loop(i * (subs // tiles), (i + 1) * (subs // tiles))
                    def _(u):
                        receive(t + 1, u)

                @pl.when(t >= 1)
                def _():
                    unit(head, i)

            @pl.when(t >= 1)
            def _():
                finish(head)

            @pl.when((t == hops - 3) | (t == hops - 2))
            def _():
                first_part(jnp.where(t == hops - 3, 1 - lax.rem(spot, 2), lax.rem(spot, 2)))

            @pl.when(t == hops - 2)
            def _():
                for way in range(2):
                    first_copy(way).start()
    else:
        @pl.loop(0, hops)
        def _(t):
            @pl.loop(0, subs)
            def _(u):
                receive(t + 1, u)

        @pl.loop(0, chips)
        def _(origin):
            shared(origin)

        @pl.loop(0, heads)
        def _(head):
            begin(head)

            for i in range(tiles):
                unit(head, i)

            finish(head)

        @pl.loop(0, 2)
        def _(way):
            first_part(way)
            first_copy(way).start()

    for way in range(2):
        first_copy(way).wait_recv()
    save_first = pltpu.make_async_copy(first_in, first_hbm, save_sem.at[groups + 1])
    save_first.start()

    for way in range(2):
        near_copy(way).wait_send()
        first_copy(way).wait_send()

    @pl.loop(1, dp_count)
    def _(k):
        swap_copy(k).wait_send()

    @pl.loop(0, subs)
    def _(u):
        @pl.loop(0, chips)
        def _(origin):
            pass_copy(origin, core, u).wait_send()

        @pl.loop(1, hops + 1)
        def _(hop):
            for way in range(2):
                @pl.when(carried(way, hop, u))
                def _():
                    forward(way, hop, u).wait_send()

    @pl.loop(0, groups)
    def _(group):
        save_copy(group).wait()

    save_tok.wait()
    save_first.wait()


def gather_attend(place, slots, tokens, queries, out_grad, seg_row, head_count, dp_count):
    slot_count = slots.shape[0]
    width = slots.shape[2] * slots.shape[3]
    tok_count = queries.shape[0]
    q_width = queries.shape[1] * queries.shape[2]
    chips = dp_count // 2
    lane = width // head_count // 2
    groups = 2 * head_count
    blocks = place.shape[0]
    splits = dp_count // groups
    rows = BR // splits
    subs = 8
    hops = chips // 2
    tile = 128
    powers = np.power(500000.0, -2.0 * np.arange(lane // 2) / lane)
    frequency = np.concatenate([powers, powers]).astype(np.float32)[None, :]
    early = (2, blocks // 2, rows, lane)
    turned = (queries.shape[1], tok_count, lane)
    bf = jnp.bfloat16
    f32 = jnp.float32
    whole = pl.BlockSpec(memory_space=pltpu.VMEM)
    far = pl.BlockSpec(memory_space=pl.ANY)
    dma = pltpu.SemaphoreType.DMA
    return pl.pallas_call(
        functools.partial(gather_kernel, chips, head_count, subs, tile),
        out_shape=(
            jax.ShapeDtypeStruct(queries.shape, bf),
            jax.ShapeDtypeStruct((tok_count, width), bf),
            jax.ShapeDtypeStruct((groups, blocks, splits, rows, lane), bf),
            jax.ShapeDtypeStruct((blocks, splits, rows, tok_count), bf),
            jax.ShapeDtypeStruct(early, bf),
        ),
        in_specs=[pl.BlockSpec(memory_space=pltpu.SMEM), whole, far, far, far, whole, whole],
        out_specs=(whole, whole, far, far, far),
        scratch_shapes=[
            pltpu.VMEM(tokens.shape, bf),
            pltpu.VMEM(turned, bf),
            pltpu.VMEM(turned, bf),
            pltpu.VMEM((2, tile // 2) + queries.shape[1:], bf),
            pltpu.VMEM((blocks, splits, rows, tok_count), bf),
            pltpu.VMEM((groups, blocks, splits, rows, lane), bf),
            pltpu.VMEM((dp_count, slot_count, rows, lane), bf),
            pltpu.VMEM((tok_count, 2 * lane), f32),
            pltpu.VMEM((tok_count, 2 * lane), bf),
            pltpu.VMEM((tok_count, tok_count), f32),
            pltpu.VMEM((lane, tok_count), bf),
            pltpu.VMEM((tok_count, lane), f32),
            pltpu.VMEM((tok_count, lane), f32),
            pltpu.VMEM((tok_count, lane), f32),
            pltpu.VMEM((tok_count, lane), f32),
            dma,
            dma((2,)),
            dma((groups + 2,)),
            dma((dp_count,)),
            dma((dp_count,)),
            dma((2, hops, subs)),
            dma((2, hops, subs)),
            dma((chips, subs)),
            dma((chips, subs)),
            pltpu.VMEM(early, bf),
            pltpu.VMEM(early, bf),
            pltpu.VMEM(early, bf),
            pltpu.VMEM(early, bf),
            dma((2,)),
            dma((2,)),
            dma((2,)),
            dma((2,)),
            pltpu.VMEM((slot_count, BR, width), bf),
        ],
        compiler_params=pltpu.CompilerParams(
            collective_id=1, has_side_effects=True, vmem_limit_bytes=VMEM_LIMIT
        ),
        cost_estimate=pl.CostEstimate(
            flops=10 * tok_count * tok_count * q_width, bytes_accessed=10**8,
            transcendentals=tok_count * tok_count * q_width // lane,
        ),
        name="gather_attend",
    )(place, slots, tokens, queries, out_grad, seg_row, frequency)


def scatter_kernel(
    chips, mp_count, subs, block_of, used, tok_hbm, pair_ref, first_ref, w_hbm, out_ref, in_ref, tok_ref,
    part_out, part_in, ring_out, ring_in, ready, final, swap_out, swap_in, wbuf, side_out, side_in,
    part_sent, part_got, ring_sent, ring_got, swap_sent, swap_got, tok_sem, load_sem, side_sent, side_got,
):
    dp_count = 2 * chips
    me, my = lax.axis_index("dp"), lax.axis_index("mp")
    core = lax.rem(me, 2)
    spot = position_of(chips, me // 2)
    ahead = 2 * chip_at(chips, lax.rem(spot + 1, chips)) + core
    behind = 2 * chip_at(chips, lax.rem(spot + chips - 1, chips)) + core
    partner = me + 1 - 2 * core
    blocks, splits, rows, tok_count = tok_ref.shape
    lane = final.shape[2]
    groups = pair_ref.shape[1] // lane
    per = chips // groups
    half = blocks // 2
    size = half // subs
    slots = swap_out.shape[1]
    keep, early = part_out.shape[1], part_out.shape[1] - 1
    deep = wbuf.shape[2]
    features = in_ref.shape[1]
    chunks = features // deep
    others, units = (mp_count - 1) * chunks, mp_count * chunks

    def load_copy(k):
        target = lax.rem(my + 1 + k // chunks, mp_count)
        start = pl.multiple_of(target * features + lax.rem(k, chunks) * deep, deep)
        slot = lax.rem(k, 2)
        return pltpu.make_async_copy(
            w_hbm.at[:, pl.ds(start, deep), :], wbuf.at[slot], load_sem.at[slot]
        )

    loads = [
        pltpu.make_async_copy(
            tok_hbm.at[pl.ds(i * half, half)], tok_ref.at[pl.ds(i * half, half)], tok_sem.at[i]
        )
        for i in range(2)
    ]
    for load in loads:
        load.start()
    load_copy(0).start()
    meet(("dp", dp_count), ("mp", mp_count))

    def goal(way, step):
        return lax.rem(spot + (chips - 1 - step if way == 0 else 1 + step), chips)

    def product(way, step, owner, u):
        position = goal(way, step)
        split = lax.rem(position, per) * 2 + owner
        left = tok_ref[way * half + u * size : way * half + (u + 1) * size, split]
        lanes = pl.ds(pl.multiple_of((position // per) * lane, lane), lane)
        return jnp.dot(
            left.reshape(size * rows, tok_count), pair_ref[:, lanes],
            preferred_element_type=jnp.float32,
        ).reshape(size, rows, lane)

    def part_copy(way, step):
        return remote(
            part_out.at[way, lax.rem(step, keep)], part_in.at[way, step],
            part_sent.at[way, step], part_got.at[way, step], partner,
        )

    def ring_copy(way, step, u):
        at = pl.ds(u * size, size)
        return remote(
            ring_out.at[way, lax.rem(step, 2), at], ring_in.at[way, step, at],
            ring_sent.at[way, step, u], ring_got.at[way, step, u],
            ahead if way == 0 else behind,
        )

    def span(u):
        return slice(u * size, (u + 1) * size)

    def part_fill(step, way, u):
        part_out[way, step % keep, span(u)] = product(way, step, 1 - core, u).astype(
            jnp.bfloat16
        )

    def ready_fill(step, way, u):
        ready[way, span(u)] = product(way, step, core, u) + part_in[way, step, span(u)].astype(
            jnp.float32
        )

    def ring_step(step, last):
        if not last:
            for way in range(2):
                part_copy(way, step + 1).wait_recv()

            @pl.when(step + early < chips)
            def _():
                for way in range(2):
                    part_copy(way, step - 1).wait_send()

        for u in range(subs):
            for way in range(2):
                ring_copy(way, step - 1, u).wait_recv()
                total = ready[way, span(u)] + ring_in[way, step - 1, span(u)].astype(jnp.float32)
                if last:
                    final[way * half + u * size : way * half + (u + 1) * size] = total.astype(
                        jnp.bfloat16
                    )
                else:
                    @pl.when(step >= 3)
                    def _():
                        ring_copy(way, step - 2, u).wait_send()

                    ring_out[way, lax.rem(step, 2), span(u)] = total.astype(jnp.bfloat16)
                    ring_copy(way, step, u).start()
                    ready_fill(step + 1, way, u)

                    @pl.when(step + early < chips)
                    def _():
                        part_fill(step + early, way, u)
        if not last:
            @pl.when(step + early < chips)
            def _():
                for way in range(2):
                    part_copy(way, step + early).start()

    def side_copy(k):
        target = lax.rem(my + 1 + k // chunks, mp_count)
        return remote(
            side_out.at[k], side_in.at[k], side_sent.at[k], side_got.at[k], target, "mp"
        )

    def unit(k):
        load_copy(k).wait()

        @pl.when(k + 1 < units)
        def _():
            load_copy(k + 1).start()

        slot = lax.rem(k, 2)
        w = jnp.concatenate([wbuf[slot, g] for g in range(groups)], axis=1)
        value = lax.dot_general(
            pair_ref[...], w, (((1,), (1,)), ((), ())), preferred_element_type=jnp.float32
        )

        @pl.when(k < others)
        def _():
            side_out[k] = value.astype(jnp.bfloat16)
            side_copy(k).start()

        @pl.when(k >= others)
        def _():
            chunk = k - others
            total = value
            for gap in range(mp_count - 1):
                side_copy(gap * chunks + chunk).wait_recv()
                total = total + side_in[gap * chunks + chunk].astype(jnp.float32)
            in_ref[:, pl.ds(pl.multiple_of(chunk * deep, deep), deep)] = total.astype(jnp.bfloat16)

    for load in loads:
        load.wait()
    for way in range(2):
        for u in range(subs):
            part_fill(1, way, u)
        part_copy(way, 1).start()
    for way in range(2):
        for u in range(subs):
            ready[way, span(u)] = product(way, 1, core, u) + first_ref[way, span(u)].astype(
                jnp.float32
            )
    for way in range(2):
        part_copy(way, 1).wait_recv()
    for u in range(subs):
        for way in range(2):
            total = ready[way, span(u)] + part_in[way, 1, span(u)].astype(jnp.float32)
            ring_out[way, 1, span(u)] = total.astype(jnp.bfloat16)
            ring_copy(way, 1, u).start()
    for step in range(2, early + 2):
        for way in range(2):
            for u in range(subs):
                part_fill(step, way, u)
            part_copy(way, step).start()
    for way in range(2):
        part_copy(way, 2).wait_recv()
        for u in range(subs):
            ready_fill(2, way, u)
    pace = 2

    @pl.loop(2, chips - 1)
    def _(step):
        ring_step(step, False)

        @pl.loop((step - 2) * pace, (step - 1) * pace)
        def _(k):
            @pl.when(k < units)
            def _():
                unit(k)

    ring_step(chips - 1, True)

    def swap_copy(k):
        peer = lax.rem(me + k, dp_count)
        return remote(swap_out.at[peer], swap_in.at[me], swap_sent.at[k], swap_got.at[k], peer)

    def fill(peer):
        for i in range(slots):
            slot = peer * slots + i
            taken = final[block_of[slot]]
            swap_out[peer, i] = jnp.where(used[slot] != 0, taken, jnp.zeros_like(taken))

    def place_in(origin, value):
        position = position_of(chips, origin // 2)
        split = lax.rem(position, per) * 2 + lax.rem(origin, 2)
        for i in range(slots):
            start = (i * BR + split * rows) * groups + position // per
            out_ref[pl.ds(start, rows, stride=groups), :] = value[i].astype(jnp.float32)

    @pl.loop(1, dp_count)
    def _(k):
        fill(lax.rem(me + k, dp_count))
        swap_copy(k).start()

    fill(me)
    place_in(me, swap_out[me])

    @pl.loop(min((chips - 3) * pace, units), units)
    def _(k):
        unit(k)

    @pl.loop(1, dp_count)
    def _(k):
        swap_copy(k).wait_recv()
        origin = lax.rem(me + dp_count - k, dp_count)
        place_in(origin, swap_in[origin])

    @pl.loop(1, dp_count)
    def _(k):
        swap_copy(k).wait_send()

    @pl.loop(0, others)
    def _(k):
        side_copy(k).wait_send()

    @pl.loop(chips - keep, chips)
    def _(step):
        for way in range(2):
            part_copy(way, step).wait_send()

    @pl.loop(chips - 3, chips - 1)
    def _(step):
        for way in range(2):
            for u in range(subs):
                ring_copy(way, step, u).wait_send()


def scatter_sum(tok_pieces, pairs, first, gathered, block_of, used, dp_count, mp_count):
    chips = dp_count // 2
    width = pairs.shape[1]
    blocks, splits, rows, tok_count = tok_pieces.shape
    groups, lane = gathered.shape[0], gathered.shape[2]
    slots = block_of.shape[0] // dp_count
    subs = 4
    keep = 4
    whole = pl.BlockSpec(memory_space=pltpu.VMEM)
    scalars = pl.BlockSpec(memory_space=pltpu.SMEM)
    far = pl.BlockSpec(memory_space=pl.ANY)
    half = blocks // 2
    features = blocks * BR // mp_count
    deep = group_of(features // BR) // 2 * BR
    others = (mp_count - 1) * features // deep
    bf = jnp.bfloat16
    dma = pltpu.SemaphoreType.DMA
    return pl.pallas_call(
        functools.partial(scatter_kernel, chips, mp_count, subs),
        out_shape=(
            jax.ShapeDtypeStruct((slots * BR * groups, lane), jnp.float32),
            jax.ShapeDtypeStruct((tok_count, features), bf),
        ),
        in_specs=[scalars, scalars, far, whole, whole, far],
        out_specs=(whole, whole),
        scratch_shapes=[
            pltpu.VMEM(tok_pieces.shape, bf),
            pltpu.VMEM((2, keep, half, rows, lane), bf),
            pltpu.VMEM((2, chips, half, rows, lane), bf),
            pltpu.VMEM((2, 2, half, rows, lane), bf),
            pltpu.VMEM((2, chips - 1, half, rows, lane), bf),
            pltpu.VMEM((2, half, rows, lane), jnp.float32),
            pltpu.VMEM((blocks, rows, lane), bf),
            pltpu.VMEM((dp_count, slots, rows, lane), bf),
            pltpu.VMEM((dp_count, slots, rows, lane), bf),
            pltpu.VMEM((2, groups, deep, lane), bf),
            pltpu.VMEM((others, tok_count, deep), bf),
            pltpu.VMEM((others, tok_count, deep), bf),
            dma((2, chips)),
            dma((2, chips)),
            dma((2, chips - 1, subs)),
            dma((2, chips - 1, subs)),
            dma((dp_count,)),
            dma((dp_count,)),
            dma((2,)),
            dma((2,)),
            dma((others,)),
            dma((others,)),
        ],
        compiler_params=pltpu.CompilerParams(
            collective_id=0, has_side_effects=True, vmem_limit_bytes=VMEM_LIMIT
        ),
        cost_estimate=pl.CostEstimate(
            flops=16 * tok_pieces.size * width, bytes_accessed=10**8, transcendentals=0
        ),
        name="scatter_sum",
    )(block_of, used, tok_pieces, pairs, first, gathered)


def local(tokens, queries, out_grad, segment_ids, weight_slots, old_place, new_place):
    tok_count = tokens.shape[0]
    slot_rows, head_count, _, head_size = weight_slots.shape
    width = head_count * 2 * head_size
    dp_count = lax.axis_size("dp")
    mp_count = lax.axis_size("mp")
    slot_total = dp_count * (slot_rows // BR)
    block_count = old_place.shape[0]

    query_grad, pair_grad, gathered, tok_pieces, first = gather_attend(
        old_place, weight_slots.reshape(slot_rows // BR, BR, 2 * head_count, head_size), tokens,
        queries, out_grad, segment_ids, head_count, dp_count,
    )
    gathered = gathered.reshape(2 * head_count, block_count * BR, head_size)

    slot_ids = jnp.arange(slot_total, dtype=jnp.int32)
    matched = (new_place[None, :] == slot_ids[:, None]).astype(jnp.int32)
    block_of = jnp.sum(matched * jnp.arange(block_count, dtype=jnp.int32)[None, :], axis=1)
    used = jnp.sum(matched, axis=1)
    weight_grad, input_grad = scatter_sum(
        tok_pieces, pair_grad, first, gathered, block_of, used, dp_count, mp_count
    )
    return (
        input_grad,
        query_grad,
        weight_grad.reshape(slot_rows, head_count, 2, head_size),
    )


def solution(mesh):
    return jax.shard_map(
        local,
        mesh=mesh,
        in_specs=(
            P("dp", None),
            P("dp", "mp", None),
            P("dp", "mp", None),
            P("dp", None),
            P("dp", "mp", None, None),
            P(),
            P(),
        ),
        out_specs=(P("dp", "mp"), P("dp", "mp", None), P("dp", "mp", None, None)),
        check_vma=False,
    )
```
